256 devices in a mesh: pass: 64 (over x, z, y_hi), cell: 4 (over y_lo, core).
Axes of the slice: x: 4, y: 4 (y_hi: 2, y_lo: 2; y = y_hi * 2 + y_lo), z: 8, core: 2. Of those that a mesh axis runs over, the one named last changes fastest.
Arguments:
- flow_state: float32 [16384, 4096], P('pass', 'cell'), may hold values from -6 to 6
- face_weights: float32 [4, 16384, 4096], P(None, 'pass', 'cell'), may hold values from 0.02 to 0.24
- forcing: float32 [16384, 4096], P('pass', 'cell'), may hold values from -1.2 to 1.2
- lagged_planes: float32 [64, 8, 4096], P('pass', None, 'cell'), may hold values from -6 to 6
- phase_lag: int32 [32, 2], replicated, may hold values from 0 to 8
- face_map: int32 [64, 4096], P('pass', 'cell'), may hold values from 0 to 4095, as said below
- surface_record: bfloat16 [64, 120, 4096], P('pass', None, 'cell'), may hold values from -6 to 6
- face_radius: float32 [2, 4096], P(None, 'cell'), may hold values from 0.3 to 1
- face_angle: float32 [2, 4096], P(None, 'cell'), may hold values from -0.3 to 0.3
- face_axial: float32 [2, 4096], P(None, 'cell'), may hold values from -0.3 to 0.3
- face_stagger: float32 [2, 4096], P(None, 'cell'), may hold values from -1.2 to 1.2
- face_area: float32 [2, 4096], P(None, 'cell'), may hold values from 0.5 to 1.5
- listeners: float32 [3, 1024], replicated, as said below
- observer_group: int32 [1024], replicated, may hold values from 0 to 15
Outputs:
- final_field: float32 [16384, 4096], P('pass', 'cell')
- acoustic: float32 [1024, 128], P('cell')
- array_signal: float32 [16, 128], replicated
The draws below stay inside these ranges and needn't reach their ends.
Inputs may be any that keep to these rules, and one draw needn't show every extreme that they name: face_map[j, a] lies in the aligned block of 1024 axial indices that holds a, and for each j the entries of a block are a permutation of that block. `listeners`: every observer is between 1.3 and 4 from the anchor.
All inputs are finite; a program needn't handle non-finite values.
Results may differ from the reference program's by a relative error of at most 0.0035.
Values sent between devices are 32-bit elements; how exact they have to be, the bound alone decides.
No kernel may reach another device: no remote copies, remote signals or barrier semaphores. Data moves between devices by JAX's collectives and lax.ppermute only.
A program may use at most 64 MiB of HBM per device.

```python
import math
import jax
import jax.numpy as jnp
from jax import lax

CA = 1024
PITCH = 512
OBS = 1024
TIMES = 128
STEPS = 8
LAGS = 8
GROUPS = 16
PASSAGES = 32
A = 4096


def draw_face_map(key, part):
    blocks = A // CA
    scores = jax.random.randint(key, (2 * PASSAGES, blocks, CA), 0, 65536)
    scores = scores * CA + jnp.arange(CA, dtype=jnp.int32)
    order = jnp.argsort(scores, axis=-1, stable=True).astype(jnp.int32)
    offsets = (jnp.arange(blocks, dtype=jnp.int32) * CA)[None, :, None]
    return (order + offsets).reshape(2 * PASSAGES, A).astype(jnp.int32)


def draw_listeners(key, part):
    first, second, third = jax.random.split(key, 3)
    polar = jax.random.uniform(first, (OBS,), jnp.float32, -1.0, 1.0)
    radius = jax.random.uniform(third, (OBS,), jnp.float32, 1.3, 4.0)
    azimuth = jax.random.uniform(second, (OBS,), jnp.float32, -math.pi, math.pi)
    lateral = jnp.sqrt(jnp.maximum(1.0 - polar * polar, 0.0))
    return jnp.stack([radius * lateral * jnp.cos(azimuth), radius * lateral * jnp.sin(azimuth), radius * polar]).astype(jnp.float32)


def set_ends(array, rng, smallest, largest):
    dims = array.shape
    index_at = [jax.random.randint(jax.random.fold_in(rng, axis), (), 0, dims[axis]) for axis in range(len(dims))]
    array = array.at[tuple(index_at)].set(smallest)
    longest = dims.index(max(dims))
    index_at[longest] = (index_at[longest] + 1) % dims[longest]
    return array.at[tuple(index_at)].set(largest)


def shard_levels(stream_key, shape, cuts, smallest, high):
    level, own = 1.0, jax.random.fold_in(stream_key, 6)
    for position, parts in cuts:
        heights = jnp.exp(jax.random.uniform(jax.random.fold_in(own, position), (parts,), jnp.float32, smallest / len(cuts), high / len(cuts)))
        level = level * jnp.repeat(heights, shape[position] // parts).reshape([-1 if axis == position else 1 for axis in range(len(shape))])
    return level


def bell_draw(rng, extent, spread, bound, cuts=(), kind=jnp.bfloat16):
    array = spread * jax.random.normal(rng, extent, jnp.float32)
    if cuts:
        array = array * shard_levels(rng, extent, cuts, -0.22, 0.18)
    return jnp.clip(array, -bound, bound).astype(kind)


def setup_inputs(seed: int = 0) -> dict:
    splits = jax.random.split(jax.random.key(seed), 15)
    return {
        "flow_state": bell_draw(splits[0], (PASSAGES * PITCH, A), 1.0, 6.0, ((0, 64), (1, 4)), jnp.float32),
        "face_weights": jnp.clip(0.02 + 0.22 * jax.random.uniform(splits[1], (4, PASSAGES * PITCH, A), jnp.float32) ** shard_levels(splits[1], (4, PASSAGES * PITCH, A), ((1, 64), (2, 4)), -0.2, 0.2), 0.02, 0.24),
        "forcing": bell_draw(splits[2], (PASSAGES * PITCH, A), 0.2, 1.2, ((0, 64), (1, 4)), jnp.float32),
        "lagged_planes": bell_draw(splits[3], (2 * PASSAGES, LAGS, A), 1.0, 6.0, ((0, 64), (2, 4)), jnp.float32),
        "phase_lag": set_ends(jax.random.randint(splits[4], (PASSAGES, 2), 0, LAGS + 1), jax.random.fold_in(splits[4], 1), 0, LAGS).astype(jnp.int32),
        "face_map": draw_face_map(jax.random.fold_in(splits[14], 71), 0),
        "surface_record": bell_draw(splits[6], (2 * PASSAGES, TIMES - STEPS, A), 1.0, 6.0, ((0, 64), (2, 4))),
        "face_radius": jnp.clip(0.3 + 0.7 * jax.random.uniform(splits[7], (2, A), jnp.float32) ** shard_levels(splits[7], (2, A), ((1, 4),), -0.2, 0.2), 0.3, 1.0),
        "face_angle": jnp.clip(jax.random.uniform(splits[8], (2, A), jnp.float32, -0.3, 0.3) * shard_levels(splits[8], (2, A), ((1, 4),), -0.4, 0.0), -0.3, 0.3),
        "face_axial": jnp.clip(jax.random.uniform(splits[9], (2, A), jnp.float32, -0.3, 0.3) * shard_levels(splits[9], (2, A), ((1, 4),), -0.4, 0.0), -0.3, 0.3),
        "face_stagger": jnp.clip(jax.random.uniform(splits[10], (2, A), jnp.float32, -1.2, 1.2) * shard_levels(splits[10], (2, A), ((1, 4),), -0.4, 0.0), -1.2, 1.2),
        "face_area": jnp.clip(0.5 + 1.0 * jax.random.uniform(splits[11], (2, A), jnp.float32) ** shard_levels(splits[11], (2, A), ((1, 4),), -0.2, 0.2), 0.5, 1.5),
        "listeners": draw_listeners(jax.random.fold_in(splits[14], 71), 0),
        "observer_group": set_ends(jax.random.randint(splits[13], (OBS,), 0, GROUPS), jax.random.fold_in(splits[13], 1), 0, GROUPS - 1).astype(jnp.int32),
    }


sound_speed = 2.0

def relax(field, coeff, forcing, ghost_low, ghost_high):
    below = jnp.concatenate([ghost_low[:, None, :], field[:, :-1, :]], axis=1)
    above = jnp.concatenate([field[:, 1:, :], ghost_high[:, None, :]], axis=1)
    border = jnp.zeros_like(field[:, :, :1])
    left = jnp.concatenate([border, field[:, :, :-1]], axis=2)
    right = jnp.concatenate([field[:, :, 1:], border], axis=2)
    keep = 1.0 - coeff[0] - coeff[1] - coeff[2] - coeff[3]
    return keep * field + coeff[0] * below + coeff[1] * above + coeff[2] * left + coeff[3] * right + forcing

def pick_level(levels, lag, mapping):
    count = levels.shape[1]
    width = levels.shape[2]
    index = jnp.broadcast_to(lag[None, :, None], (1, count, width)).astype(jnp.int32)
    chosen = jnp.take_along_axis(levels, index, axis=0)[0]
    return jnp.take_along_axis(chosen, mapping.astype(jnp.int32), axis=1)

def time_rate(signal, axis):
    values = signal.astype(jnp.float32)
    length = values.shape[axis]
    inner = (lax.slice_in_dim(values, 2, length, axis=axis) - lax.slice_in_dim(values, 0, length - 2, axis=axis)) * 0.5
    head = lax.slice_in_dim(values, 1, 2, axis=axis) - lax.slice_in_dim(values, 0, 1, axis=axis)
    tail = lax.slice_in_dim(values, length - 1, length, axis=axis) - lax.slice_in_dim(values, length - 2, length - 1, axis=axis)
    return jnp.concatenate([head, inner, tail], axis=axis).astype(jnp.bfloat16)

def kernel_pair(points, theta, radius, angle, axial, stagger, area, scale):
    phase = theta + angle
    cos_phase = jnp.cos(phase)
    sin_phase = jnp.sin(phase)
    normal_x = -jnp.cos(stagger) * sin_phase
    normal_y = jnp.cos(stagger) * cos_phase
    normal_z = jnp.sin(stagger)
    delta_x = points[0][:, None] - (radius * cos_phase)[None, :]
    delta_y = points[1][:, None] - (radius * sin_phase)[None, :]
    delta_z = points[2][:, None] - axial[None, :]
    dist_sq = delta_x * delta_x + delta_y * delta_y + delta_z * delta_z
    dist = jnp.sqrt(dist_sq)
    cosine = (normal_x[None, :] * delta_x + normal_y[None, :] * delta_y + normal_z[None, :] * delta_z) / dist
    weight = (area * scale / (4.0 * math.pi))[None, :] * cosine
    press = (weight / dist_sq).astype(jnp.bfloat16)
    change = (weight / (sound_speed * dist)).astype(jnp.bfloat16)
    return jnp.concatenate([press, change], axis=1)

def reference(flow_state, face_weights, forcing, lagged_planes, phase_lag, face_map, surface_record, face_radius, face_angle, face_axial, face_stagger, face_area, listeners, observer_group):
    field = flow_state.reshape(PASSAGES, PITCH, A)
    coeff = face_weights.reshape(4, PASSAGES, PITCH, A)
    push = forcing.reshape(PASSAGES, PITCH, A)
    planes = lagged_planes.reshape(PASSAGES, 2, LAGS, A)
    maps = face_map.reshape(PASSAGES, 2, A)
    lower_levels = jnp.concatenate([field[None, :, 0, :], jnp.moveaxis(planes[:, 0], 1, 0)], axis=0)
    upper_levels = jnp.concatenate([field[None, :, -1, :], jnp.moveaxis(planes[:, 1], 1, 0)], axis=0)
    surfaces = []
    for level in range(STEPS):
        ghost_low = pick_level(jnp.roll(upper_levels, 1, axis=1), phase_lag[:, 0], maps[:, 0, :])
        ghost_high = pick_level(jnp.roll(lower_levels, -1, axis=1), phase_lag[:, 1], maps[:, 1, :])
        field = relax(field, coeff, push, ghost_low, ghost_high)
        lower_levels = jnp.concatenate([field[None, :, 0, :], lower_levels[:-1]], axis=0)
        upper_levels = jnp.concatenate([field[None, :, -1, :], upper_levels[:-1]], axis=0)
        sides = jnp.stack([field[:, PITCH // 4, :], field[:, PITCH // 4 + PITCH // 2, :]], axis=1)
        surfaces.append(sides.reshape(2 * PASSAGES, A).astype(jnp.bfloat16))
    surface = jnp.concatenate([surface_record, jnp.stack(surfaces, axis=1)], axis=1)
    rate = time_rate(surface, 1)
    rows = jnp.arange(2 * PASSAGES, dtype=jnp.int32)
    thetas = (rows // 2).astype(jnp.float32) * (2.0 * math.pi / PASSAGES)
    side_ids = (rows % 2).astype(jnp.int32)
    scale = 64.0 / math.sqrt(2 * A * PASSAGES)

    def passage_term(operands):
        signal, change, theta, side = operands
        kernel = kernel_pair(listeners, theta, face_radius[side], face_angle[side], face_axial[side], face_stagger[side], face_area[side], scale)
        data = jnp.concatenate([signal, change], axis=1)
        return jnp.dot(kernel, data.T, preferred_element_type=jnp.float32)
    terms = lax.map(passage_term, (surface, rate, thetas, side_ids))
    acoustic = lax.optimization_barrier(jnp.sum(terms, axis=0))
    member = (observer_group[None, :] == jnp.arange(GROUPS, dtype=jnp.int32)[:, None]).astype(jnp.float32)
    counts = lax.optimization_barrier(jnp.sum(member, axis=1))
    totals = jnp.dot(member, acoustic, precision=lax.Precision.HIGHEST, preferred_element_type=jnp.float32)
    array_signal = totals / jnp.maximum(counts, 1.0)[:, None]
    return (field.reshape(PASSAGES * PITCH, A), acoustic, array_signal)
```

```python
import functools
import math

import jax
import jax.numpy as jnp
from jax import lax
from jax.experimental import pallas as pl
from jax.experimental.pallas import tpu as pltpu
from jax.sharding import Mesh
from jax.sharding import PartitionSpec as P

STEPS = 8
GROUPS = 16
sound_speed = 2.0

W = 1024
E = 128
WX = W + E
TOP = 16 + 256
ROWS = TOP + 16
SPLIT = {"x": 4, "z": 8, "y_hi": 2}
PASS = ("x", "z", "y_hi")
VMEM_LIMIT = 24 * 1024 * 1024
F32 = jnp.float32


def params(**kw):
    return pltpu.CompilerParams(vmem_limit_bytes=VMEM_LIMIT, **kw)


def vmem():
    return pl.BlockSpec(memory_space=pltpu.VMEM)


def smem():
    return pl.BlockSpec(memory_space=pltpu.SMEM)


def place():
    index = lax.axis_index("x") * (SPLIT["z"] * SPLIT["y_hi"]) + lax.axis_index("z") * SPLIT["y_hi"]
    index = index + lax.axis_index("y_hi")
    return index // 2, index % 2


def strips_body(field, weights, forcing, lagged, maps, to_mid, to_plane, sems):
    _, half = place()
    mid = pl.multiple_of(jnp.where(half == 0, 248, 0), 8)
    plane = pl.multiple_of(jnp.where(half == 0, 0, 248), 8)
    copies = []
    for out, start in ((to_mid, mid), (to_plane, plane)):
        rows = pl.ds(start, 8)
        copies.append((field.at[rows], out.at[pl.ds(0, 8)]))
        for i in range(4):
            copies.append((weights.at[i, rows], out.at[pl.ds(8 + 8 * i, 8)]))
        copies.append((forcing.at[rows], out.at[pl.ds(40, 8)]))
    copies.append((lagged.at[0], to_plane.at[pl.ds(48, 8)]))
    started = []
    for n, (source, target) in enumerate(copies):
        copy = pltpu.make_async_copy(source, target, sems.at[n])
        copy.start()
        started.append(copy)
    to_plane[56:64, :] = jnp.broadcast_to(maps[...].astype(F32), (8, W))
    for copy in started:
        copy.wait()


def strips(field, weights, forcing, lagged, maps):
    anywhere = pl.BlockSpec(memory_space=pl.ANY)
    return pl.pallas_call(
        strips_body,
        out_shape=(jax.ShapeDtypeStruct((48, W), F32), jax.ShapeDtypeStruct((64, W), F32)),
        in_specs=[anywhere, anywhere, anywhere, anywhere, vmem()],
        out_specs=(vmem(), vmem()),
        scratch_shapes=[pltpu.SemaphoreType.DMA((13,))],
        compiler_params=params(),
        name="strips",
    )(field, weights, forcing, lagged, maps)


def square(row):
    tiles = [row[:, 128 * s : 128 * (s + 1)] for s in range(8)]
    return jnp.concatenate(tiles, axis=0).astype(jnp.int32) & (W - 1)


def level_row(level):
    return jnp.where(level >= 0, 8 + level, -level - 1)


def picked(history, level, index):
    row = level_row(level)
    high, low = index >> 7, index & 127
    tiles = history[row]
    out = jnp.zeros((8, 128), F32)
    for b in range(8):
        source = jnp.broadcast_to(tiles[b : b + 1, :], (8, 128))
        value = jnp.take_along_axis(source, low, axis=1, mode="promise_in_bounds")
        out = jnp.where(high == b, value, out)
    return out


def keep_row(history, row, array, at):
    for b in range(8):
        history[row, b : b + 1, :] = array[at : at + 1, 128 * b : 128 * (b + 1)]


def keep_lagged(history, lagged):
    for j in range(8):
        for b in range(8):
            history[j, b : b + 1, :] = lagged[j : j + 1, 128 * b : 128 * (b + 1)]


def put_row(array, row, value):
    for s in range(8):
        array[row : row + 1, 128 * s : 128 * (s + 1)] = value[s : s + 1, :]


def fill_gaps(array, own, other, index, lags, half, level):
    main = pl.ds(0, W)

    @pl.when(half == 0)
    def _():
        keep_row(own, 8 + level, array, 16)
        keep_row(other, 8 + level, array, 7)

    @pl.when(half == 1)
    def _():
        keep_row(own, 8 + level, array, TOP - 1)
        keep_row(other, 8 + level, array, TOP + 8)

    mine = picked(other, level - lags[0], index[0])
    theirs = picked(own, level - lags[1], index[1])

    @pl.when(half == 0)
    def _():
        put_row(array, 15, mine)
        put_row(array, 8, theirs)
        array[TOP : TOP + 1, main] = array[TOP + 8 : TOP + 9, main]
        array[TOP + 7 : TOP + 8, main] = array[TOP - 1 : TOP, main]

    @pl.when(half == 1)
    def _():
        put_row(array, TOP, mine)
        put_row(array, TOP + 7, theirs)
        array[15:16, main] = array[7:8, main]
        array[8:9, main] = array[16:17, main]


def lag_pair(phase_lag, passage, half):
    count = phase_lag.shape[0]
    beside = lax.rem(passage + 2 * half - 1 + count, count)
    return phase_lag[passage, half], phase_lag[beside, 1 - half]


def relaxed(current, before, after, weights, forcing, width):
    sub = lax.broadcasted_iota(jnp.int32, (8, width), 0)
    inner = current[:, :width]
    below = jnp.where(sub == 0, pltpu.roll(before[:, :width], 1, 0), pltpu.roll(inner, 1, 0))
    above = jnp.where(sub == 7, pltpu.roll(after[:, :width], 7, 0), pltpu.roll(inner, 7, 0))
    left = pltpu.roll(current, 1, 1)[:, :width]
    right = pltpu.roll(current, WX - 1, 1)[:, :width]
    low = weights[0] * (below - inner) + weights[1] * (above - inner)
    side = weights[2] * (left - inner) + weights[3] * (right - inner)
    return (inner + forcing) + (low + side)


def step(source, target, weights, forcing, strip, rim, width, strips_too):
    def joined(own, edge):
        return own if width == W else jnp.concatenate([own, edge], axis=1)

    def one(start, row):
        own = pl.ds(row, 8)
        at = pl.ds(start, 8)
        w = [joined(weights[i, own, :], rim[i, at, :]) for i in range(4)]
        f = joined(forcing[own, :], rim[4, at, :])
        new = relaxed(
            source[at, :], source[pl.ds(start - 8, 8), :], source[pl.ds(start + 8, 8), :], w, f, width
        )
        return new

    def tile(t, carry):
        row = pl.multiple_of(8 * t, 8)
        start = pl.multiple_of(16 + 8 * t, 8)
        new = one(start, row)
        if target.shape[0] == ROWS:
            target[pl.ds(start, 8), :width] = new
        else:
            target[pl.ds(row, 8), :width] = new
        return carry

    lax.fori_loop(0, 32, tile, 0, unroll=2)
    if strips_too:
        for start, first, before, after in ((0, 0, 0, 8), (ROWS - 8, 8, ROWS - 16, ROWS - 8)):
            at = slice(start, start + 8)
            w = [joined(strip[i, first : first + 8, :], rim[i, at, :]) for i in range(4)]
            f = joined(strip[4, first : first + 8, :], rim[4, at, :])
            target[at, :width] = relaxed(
                source[at, :], source[before : before + 8, :], source[after : after + 8, :], w, f, width
            )


def strip_tiles(from_mid, from_plane, half, row, lanes):
    mid = from_mid[row : row + 8, lanes]
    plane = from_plane[row : row + 8, lanes]
    return jnp.where(half == 0, plane, mid), jnp.where(half == 0, mid, plane)


def edges_body(
    first, last, u_l, u_r, w_l, w_r, f_l, f_r, lagged, maps, from_mid, from_plane, phase_lag, to_left, to_right,
    array, own, other,
):
    passage, half = place()
    full = slice(0, W)
    bottom, top = strip_tiles(from_mid, from_plane, half, 0, full)
    array[0:8, :] = bottom
    array[ROWS - 8 : ROWS, :] = top
    array[16:24, :] = first[...]
    array[TOP - 8 : TOP, :] = last[...]
    array[8:16, :] = jnp.zeros((8, W), F32)
    array[TOP : TOP + 8, :] = jnp.zeros((8, W), F32)
    keep_lagged(own, lagged.at[0])
    keep_lagged(other, from_plane.at[48:56])
    index = (square(maps[...]), square(from_plane[56:57, :]))
    fill_gaps(array, own, other, index, lag_pair(phase_lag, passage, half), half, 0)

    for out, block, u, w, f, sign in ((to_left, 0, u_l, w_l, f_l, 1), (to_right, 7, u_r, w_r, f_r, -1)):
        lanes = slice(128 * block, 128 * (block + 1))

        def packed(value, extra):
            lane = lax.broadcasted_iota(jnp.int32, value.shape, 1)
            for i, e in enumerate(extra):
                spot = 2 + i if sign == 1 else 125 - i
                value = jnp.where(lane == spot, pltpu.roll(e, (sign * (2 + i)) % 128, 1), value)
            return value

        out[16:TOP, :] = packed(u[...], [w[0], w[1], w[2], w[3], f[...]])
        pairs = [strip_tiles(from_mid, from_plane, half, 8 * i, lanes) for i in range(6)]
        out[0:8, :] = packed(pairs[0][0], [p[0] for p in pairs[1:]])
        out[ROWS - 8 : ROWS, :] = packed(pairs[0][1], [p[1] for p in pairs[1:]])
        out[8:16, :] = array[8:16, lanes]
        out[TOP : TOP + 8, :] = array[TOP : TOP + 8, lanes]


def edges(field, weights, forcing, lagged, maps, from_mid, from_plane, phase_lag):
    def spec(shape, *at):
        return pl.BlockSpec(shape, lambda i: at)

    whole = [spec((1, 8, W), 0, 0, 0), spec((1, W), 0, 0), spec((48, W), 0, 0), spec((64, W), 0, 0), smem()]
    return pl.pallas_call(
        edges_body,
        grid=(1,),
        out_shape=(jax.ShapeDtypeStruct((ROWS, E), F32),) * 2,
        in_specs=[
            spec((8, W), 0, 0),
            spec((8, W), 31, 0),
            spec((256, E), 0, 0),
            spec((256, E), 0, 7),
            spec((4, 256, E), 0, 0, 0),
            spec((4, 256, E), 0, 0, 7),
            spec((256, E), 0, 0),
            spec((256, E), 0, 7),
            *whole,
        ],
        out_specs=(spec((ROWS, E), 0, 0),) * 2,
        scratch_shapes=[pltpu.VMEM((ROWS, W), F32), pltpu.VMEM((16, 8, 128), F32), pltpu.VMEM((16, 8, 128), F32)],
        compiler_params=params(),
        name="edges",
    )(field, field, field, field, weights, weights, forcing, forcing, lagged, maps, from_mid, from_plane, phase_lag)


def set_rim(array, from_left, from_right):
    lane = lax.broadcasted_iota(jnp.int32, (ROWS, E), 1)
    array[:, W:] = jnp.where(lane < 64, from_right[...], from_left[...])


def finish(level, source, between, out, surface, weights, forcing, strip, rim, own, other, index, lags, half, tail):
    step(source, between, weights, forcing, strip, rim, WX, True)
    surface[0:1, :] = between[16 + 128 : 17 + 128, :W]
    fill_gaps(between, own, other, index, lags, half, level + 1)
    step(between, out, weights, forcing, strip, rim, W, not tail)
    row = 128 if tail else 16 + 128
    surface[1:2, :] = out[row : row + 1, :]
    surface[2:8, :] = jnp.zeros((6, W), F32)


def first_body(
    field, weights, forcing, lagged, maps, from_mid, from_plane, from_left, from_right, phase_lag,
    out, to_left, to_right, surface, own, other, strip, rim, index, source, between,
):
    passage, half = place()
    full = slice(0, W)
    bottom, top = strip_tiles(from_mid, from_plane, half, 0, full)
    source[0:8, :W] = bottom
    source[ROWS - 8 : ROWS, :W] = top
    source[16:TOP, :W] = field[...]
    source[8:16, :W] = jnp.zeros((8, W), F32)
    source[TOP : TOP + 8, :W] = jnp.zeros((8, W), F32)
    set_rim(source, from_left, from_right)
    lane = lax.broadcasted_iota(jnp.int32, (ROWS, E), 1)
    for i in range(5):
        bottom, top = strip_tiles(from_mid, from_plane, half, 8 + 8 * i, full)
        strip[i, 0:8, :] = bottom
        strip[i, 8:16, :] = top
        right = pltpu.roll(from_right[...], 128 - (2 + i), 1)
        left = pltpu.roll(from_left[...], 2 + i, 1)
        rim[i, :, :] = jnp.where(lane == 0, right, jnp.where(lane == 127, left, 0.0))
    keep_lagged(own, lagged.at[0])
    keep_lagged(other, from_plane.at[48:56])
    own[8:16] = jnp.zeros((8, 8, 128), F32)
    other[8:16] = jnp.zeros((8, 8, 128), F32)
    index[0:8, :] = square(maps[...])
    index[8:16, :] = square(from_plane[56:57, :])
    pair = (index[0:8, :], index[8:16, :])
    lags = lag_pair(phase_lag, passage, half)
    fill_gaps(source, own, other, pair, lags, half, 0)
    out[8:16, :] = jnp.zeros((8, W), F32)
    out[TOP : TOP + 8, :] = jnp.zeros((8, W), F32)
    between[8:16, :] = jnp.zeros((8, WX), F32)
    between[TOP : TOP + 8, :] = jnp.zeros((8, WX), F32)
    finish(0, source, between, out, surface, weights, forcing, strip, rim, own, other, pair, lags, half, False)
    fill_gaps(out, own, other, pair, lags, half, 2)
    to_left[...] = out[:, :E]
    to_right[...] = out[:, W - E :]


def next_body(
    level, tail, state, weights, forcing, from_left, from_right, own_in, other_in, strip, rim, index, phase_lag, *rest
):
    if tail:
        out, surface, own, other, source, between = rest
    else:
        out, to_left, to_right, surface, own, other, source, between = rest
    passage, half = place()
    own[...] = own_in[...]
    other[...] = other_in[...]
    source[:, :W] = state[...]
    set_rim(source, from_left, from_right)
    between[8:16, :] = jnp.zeros((8, WX), F32)
    between[TOP : TOP + 8, :] = jnp.zeros((8, WX), F32)
    pair = (index[0:8, :], index[8:16, :])
    lags = lag_pair(phase_lag, passage, half)
    finish(level, source, between, out, surface, weights, forcing, strip, rim, own, other, pair, lags, half, tail)
    if not tail:
        out[8:16, :] = jnp.zeros((8, W), F32)
        out[TOP : TOP + 8, :] = jnp.zeros((8, W), F32)
        fill_gaps(out, own, other, pair, lags, half, level + 2)
        to_left[...] = out[:, :E]
        to_right[...] = out[:, W - E :]


HISTORY = jax.ShapeDtypeStruct((16, 8, 128), F32)
EDGE = jax.ShapeDtypeStruct((ROWS, E), F32)
STATE = jax.ShapeDtypeStruct((ROWS, W), F32)
BUFFERS = [pltpu.VMEM((ROWS, WX), F32), pltpu.VMEM((ROWS, WX), F32)]
COST = pl.CostEstimate(flops=2 * 16 * 330 * 1024, bytes_accessed=8 << 20, transcendentals=0)


def first_steps(field, weights, forcing, lagged, maps, from_mid, from_plane, from_left, from_right, phase_lag):
    outs = (
        STATE, EDGE, EDGE, jax.ShapeDtypeStruct((8, W), F32), HISTORY, HISTORY,
        jax.ShapeDtypeStruct((5, 16, W), F32), jax.ShapeDtypeStruct((5, ROWS, E), F32),
        jax.ShapeDtypeStruct((16, 128), jnp.int32),
    )
    return pl.pallas_call(
        first_body,
        out_shape=outs,
        in_specs=[vmem()] * 9 + [smem()],
        out_specs=tuple(vmem() for _ in outs),
        scratch_shapes=BUFFERS,
        compiler_params=params(),
        cost_estimate=COST,
        name="steps_first",
    )(field, weights, forcing, lagged, maps, from_mid, from_plane, from_left, from_right, phase_lag)


def next_steps(level, state, weights, forcing, from_left, from_right, own, other, strip, rim, index, phase_lag):
    tail = level == STEPS - 2
    surface = jax.ShapeDtypeStruct((8, W), F32)
    if tail:
        outs = (jax.ShapeDtypeStruct((256, W), F32), surface)
        scratch = [pltpu.VMEM((16, 8, 128), F32), pltpu.VMEM((16, 8, 128), F32), *BUFFERS]
    else:
        outs = (STATE, EDGE, EDGE, surface, HISTORY, HISTORY)
        scratch = BUFFERS
    return pl.pallas_call(
        functools.partial(next_body, level, tail),
        out_shape=outs,
        in_specs=[vmem()] * 10 + [smem()],
        out_specs=tuple(vmem() for _ in outs),
        scratch_shapes=scratch,
        compiler_params=params(),
        cost_estimate=COST,
        name=f"steps_{level}",
    )(state, weights, forcing, from_left, from_right, own, other, strip, rim, index, phase_lag)


def kernels_body(points, radius, angle, axial, stagger, area, press, change, *, scale, passages):
    passage, half = place()

    def mine(ref):
        return jnp.where(half == 0, ref[0:1, :], ref[1:2, :])

    phase = passage.astype(F32) * (2.0 * math.pi / passages) + mine(angle)
    cos_phase, sin_phase = jnp.cos(phase), jnp.sin(phase)
    cos_stagger = jnp.cos(mine(stagger))
    weight = mine(area) * (scale / (4.0 * math.pi))
    normal_x = -weight * cos_stagger * sin_phase
    normal_y = weight * cos_stagger * cos_phase
    normal_z = weight * jnp.sin(mine(stagger))
    face_x = mine(radius) * cos_phase
    face_y = mine(radius) * sin_phase
    face_z = mine(axial)

    def tile(t, carry):
        rows = pl.ds(pl.multiple_of(16 * t, 16), 16)
        at = points[rows, :]
        delta_x = at[:, 0:1] - face_x
        delta_y = at[:, 1:2] - face_y
        delta_z = at[:, 2:3] - face_z
        inverse = lax.rsqrt(delta_x * delta_x + delta_y * delta_y + delta_z * delta_z)
        along = normal_x * delta_x + normal_y * delta_y + normal_z * delta_z
        both = along * inverse * inverse
        press[rows, :] = (both * inverse).astype(jnp.bfloat16)
        change[rows, :] = (both * (1.0 / sound_speed)).astype(jnp.bfloat16)
        return carry

    lax.fori_loop(0, press.shape[0] // 16, tile, 0)


def kernels(points, radius, angle, axial, stagger, area, part, count, scale, passages):
    size = points.shape[0] // count
    faces = pl.BlockSpec((2, W), lambda i: (0, 0))
    shape = jax.ShapeDtypeStruct((size, W), jnp.bfloat16)
    return pl.pallas_call(
        functools.partial(kernels_body, scale=scale, passages=passages),
        grid=(1,),
        out_shape=(shape, shape),
        in_specs=[pl.BlockSpec((size, 3), lambda i: (part, 0))] + [faces] * 5,
        out_specs=(pl.BlockSpec((size, W), lambda i: (0, 0)),) * 2,
        compiler_params=params(),
        cost_estimate=pl.CostEstimate(flops=20 * size * W, bytes_accessed=4 * size * W, transcendentals=size * W),
        name=f"kernels_{part}",
    )(points, radius, angle, axial, stagger, area)


def sound_body(*refs):
    presses, changes, (record, s0, s1, s2, s3, group, out, total) = refs[:4], refs[4:8], refs[8:]
    late = jnp.concatenate([s[0:2, :] for s in (s0, s1, s2, s3)], axis=0).astype(jnp.bfloat16)
    surface = jnp.concatenate([record[0].astype(F32), late.astype(F32)], axis=0)
    times = surface.shape[0]
    row = lax.broadcasted_iota(jnp.int32, surface.shape, 0)
    after, before = pltpu.roll(surface, times - 1, 0), pltpu.roll(surface, 1, 0)
    first = row == 0
    last = row == times - 1
    rate = jnp.where(last, surface, after) - jnp.where(first, surface, before)
    rate = jnp.where(first | last, rate, rate * 0.5).astype(jnp.bfloat16)
    surface = surface.astype(jnp.bfloat16)
    turned = (((1,), (1,)), ((), ()))
    size = presses[0].shape[0]
    for n in range(4):
        got = lax.dot_general(presses[n][...], surface, turned, preferred_element_type=F32)
        got = got + lax.dot_general(changes[n][...], rate, turned, preferred_element_type=F32)
        total[size * n : size * (n + 1), :] = got
    label = lax.broadcasted_iota(jnp.int32, (GROUPS, group.shape[1]), 0)
    member = (group[...] == label).astype(F32)
    counts = jnp.sum(member, axis=1, keepdims=True)
    means = jnp.dot(member, total[...], precision=lax.Precision.HIGHEST, preferred_element_type=F32)
    means = means / jnp.maximum(counts, 1.0)
    for s in range(8):
        for c in range(4):
            start = 256 * c + 32 * s
            out[4 * s + c, 0:32, :] = total[start : start + 32, :]
            out[4 * s + c, 32:34, :] = means[2 * s : 2 * s + 2, :]
            out[4 * s + c, 34:40, :] = jnp.zeros((6, 128), F32)


def sound(presses, changes, record, surfaces, group):
    return pl.pallas_call(
        sound_body,
        out_shape=jax.ShapeDtypeStruct((32, 40, 128), F32),
        in_specs=[vmem()] * 14,
        out_specs=vmem(),
        scratch_shapes=[pltpu.VMEM((1024, 128), F32)],
        compiler_params=params(),
        name="sound",
    )(*presses, *changes, record, *surfaces, group)


def exchanged(pieces, axes):
    return lax.all_to_all(pieces, axes, 0, 0, tiled=True)


def sent_to_all(block, axes):
    count = lax.axis_size(axes)
    return exchanged(jnp.broadcast_to(block, (count, *block.shape)), axes)


def on_device(
    flow_state,
    face_weights,
    forcing,
    lagged_planes,
    phase_lag,
    face_map,
    surface_record,
    face_radius,
    face_angle,
    face_axial,
    face_stagger,
    face_area,
    listeners,
    observer_group,
):
    passes = lax.axis_size(PASS)
    cells = lax.axis_size("cell")
    scale = 64.0 / math.sqrt(W * cells * passes)
    across = [(i, i ^ 1) for i in range(passes)]
    over = [(i, ((i + 1) ^ 1) - 1 if 0 < i < passes - 1 else passes - 1 - i) for i in range(passes)]
    rightward = [(i, i + 1) for i in range(cells - 1)]
    leftward = [(i + 1, i) for i in range(cells - 1)]

    to_mid, to_plane = strips(flow_state, face_weights, forcing, lagged_planes, face_map)
    from_mid = lax.ppermute(to_mid, PASS, across)
    from_plane = lax.ppermute(to_plane, PASS, over)

    points = listeners.T
    pairs = [
        kernels(points, face_radius, face_angle, face_axial, face_stagger, face_area, n, 4, scale, passes // 2)
        for n in range(4)
    ]

    to_left, to_right = edges(
        flow_state, face_weights, forcing, lagged_planes, face_map, from_mid, from_plane, phase_lag
    )
    from_left = lax.ppermute(to_right, "cell", rightward)
    from_right = lax.ppermute(to_left, "cell", leftward)
    state, to_left, to_right, surface, own, other, strip, rim, index = first_steps(
        flow_state, face_weights, forcing, lagged_planes, face_map, from_mid, from_plane, from_left, from_right,
        phase_lag,
    )
    surfaces = [surface]
    for level in range(2, STEPS, 2):
        from_left = lax.ppermute(to_right, "cell", rightward)
        from_right = lax.ppermute(to_left, "cell", leftward)
        got = next_steps(
            level, state, face_weights, forcing, from_left, from_right, own, other, strip, rim, index, phase_lag
        )
        if level < STEPS - 2:
            state, to_left, to_right, surface, own, other = got
        else:
            state, surface = got
        surfaces.append(surface)

    pieces = sound(
        [p[0] for p in pairs], [p[1] for p in pairs], surface_record, surfaces, observer_group[None, :]
    )
    part = jnp.sum(exchanged(pieces, ("x", "y_hi", "cell")), axis=0)
    part = jnp.sum(sent_to_all(part, "z"), axis=0)
    parts = sent_to_all(part, ("x", "y_hi"))
    acoustic = parts[:, :32].reshape(256, 128)
    array_signal = parts[:, 32:34].reshape(GROUPS, 128)
    return state, acoustic, array_signal


def solution(mesh):
    sizes = tuple(SPLIT.values())
    fine = Mesh(mesh.devices.reshape(*sizes, mesh.shape["cell"]), (*PASS, "cell"))
    return jax.shard_map(
        on_device,
        mesh=fine,
        in_specs=(
            P(PASS, "cell"),
            P(None, PASS, "cell"),
            P(PASS, "cell"),
            P(PASS, None, "cell"),
            P(),
            P(PASS, "cell"),
            P(PASS, None, "cell"),
            P(None, "cell"),
            P(None, "cell"),
            P(None, "cell"),
            P(None, "cell"),
            P(None, "cell"),
            P(),
            P(),
        ),
        out_specs=(P(PASS, "cell"), P("cell", None), P()),
        check_vma=False,
    )
```

```python
import functools
import math

import jax
import jax.numpy as jnp
from jax import lax
from jax.experimental import pallas as pl
from jax.experimental.pallas import tpu as pltpu
from jax.sharding import Mesh
from jax.sharding import PartitionSpec as P

STEPS = 8
GROUPS = 16
sound_speed = 2.0

W = 1024
E = 128
WX = W + E
TOP = 16 + 256
ROWS = TOP + 16
PACKED = 24
SPLIT = {"x": 4, "z": 8, "y_hi": 2}
PASS = ("x", "z", "y_hi")
VMEM_LIMIT = 8 * 1024 * 1024
F32 = jnp.float32
EDGE = jax.ShapeDtypeStruct((PACKED, E), F32)


def params(**kw):
    return pltpu.CompilerParams(vmem_limit_bytes=VMEM_LIMIT, **kw)


def vmem():
    return pl.BlockSpec(memory_space=pltpu.VMEM)


def smem():
    return pl.BlockSpec(memory_space=pltpu.SMEM)


def place():
    index = lax.axis_index("x") * (SPLIT["z"] * SPLIT["y_hi"]) + lax.axis_index("z") * SPLIT["y_hi"]
    index = index + lax.axis_index("y_hi")
    return index // 2, index % 2


def strips_body(field, weights, forcing, lagged, maps, to_mid, to_plane, sems):
    _, half = place()
    mid = pl.multiple_of(jnp.where(half == 0, 248, 0), 8)
    plane = pl.multiple_of(jnp.where(half == 0, 0, 248), 8)
    copies = []
    for out, start in ((to_mid, mid), (to_plane, plane)):
        rows = pl.ds(start, 8)
        copies.append((field.at[rows], out.at[pl.ds(0, 8)]))
        for i in range(4):
            copies.append((weights.at[i, rows], out.at[pl.ds(8 + 8 * i, 8)]))
        copies.append((forcing.at[rows], out.at[pl.ds(40, 8)]))
    copies.append((lagged.at[0], to_plane.at[pl.ds(48, 8)]))
    started = []
    for n, (source, target) in enumerate(copies):
        copy = pltpu.make_async_copy(source, target, sems.at[n])
        copy.start()
        started.append(copy)
    to_plane[56:64, :] = jnp.broadcast_to(maps[...].astype(F32), (8, W))
    for copy in started:
        copy.wait()


def strips(field, weights, forcing, lagged, maps):
    anywhere = pl.BlockSpec(memory_space=pltpu.HBM)
    return pl.pallas_call(
        strips_body,
        out_shape=(jax.ShapeDtypeStruct((48, W), F32), jax.ShapeDtypeStruct((64, W), F32)),
        in_specs=[anywhere, anywhere, anywhere, anywhere, vmem()],
        out_specs=(vmem(), vmem()),
        scratch_shapes=[pltpu.SemaphoreType.DMA((13,))],
        compiler_params=params(),
        name="strips",
    )(field, weights, forcing, lagged, maps)


def load_body(*refs):
    count = (len(refs) - 1) // 2
    copies = [pltpu.make_async_copy(refs[n], refs[count + n], refs[-1].at[n]) for n in range(count)]
    for copy in copies:
        copy.start()
    for copy in copies:
        copy.wait()


def load(arrays):
    count = len(arrays)
    return pl.pallas_call(
        load_body,
        out_shape=tuple(jax.ShapeDtypeStruct(a.shape, a.dtype) for a in arrays),
        in_specs=[pl.BlockSpec(memory_space=pltpu.HBM)] * count,
        out_specs=(vmem(),) * count,
        scratch_shapes=[pltpu.SemaphoreType.DMA((count,))],
        compiler_params=params(),
        cost_estimate=pl.CostEstimate(flops=0, bytes_accessed=12 << 20, transcendentals=0),
        name="load",
    )(*arrays)


def square(row):
    tiles = [row[:, 128 * s : 128 * (s + 1)] for s in range(8)]
    return jnp.concatenate(tiles, axis=0).astype(jnp.int32) & (W - 1)


def level_row(level):
    return jnp.where(level >= 0, 8 + level, -level - 1)


def picked(history, level, index):
    row = level_row(level)
    high, low = index >> 7, index & 127
    tiles = history[row]
    out = jnp.zeros((8, 128), F32)
    for b in range(8):
        source = jnp.broadcast_to(tiles[b : b + 1, :], (8, 128))
        value = jnp.take_along_axis(source, low, axis=1, mode="promise_in_bounds")
        out = jnp.where(high == b, value, out)
    return out


def keep_row(history, row, array, at):
    for b in range(8):
        history[row, b : b + 1, :] = array[at : at + 1, 128 * b : 128 * (b + 1)]


def keep_lagged(history, lagged):
    for j in range(8):
        for b in range(8):
            history[j, b : b + 1, :] = lagged[j : j + 1, 128 * b : 128 * (b + 1)]


def put_row(array, row, value):
    for s in range(8):
        array[row : row + 1, 128 * s : 128 * (s + 1)] = value[s : s + 1, :]


def fill_gaps(array, own, other, index, lags, half, level):
    main = pl.ds(0, W)

    @pl.when(half == 0)
    def _():
        keep_row(own, 8 + level, array, 16)
        keep_row(other, 8 + level, array, 7)

    @pl.when(half == 1)
    def _():
        keep_row(own, 8 + level, array, TOP - 1)
        keep_row(other, 8 + level, array, TOP + 8)

    mine = picked(other, level - lags[0], index[0])
    theirs = picked(own, level - lags[1], index[1])

    @pl.when(half == 0)
    def _():
        put_row(array, 15, mine)
        put_row(array, 8, theirs)
        array[TOP : TOP + 1, main] = array[TOP + 8 : TOP + 9, main]
        array[TOP + 7 : TOP + 8, main] = array[TOP - 1 : TOP, main]

    @pl.when(half == 1)
    def _():
        put_row(array, TOP, mine)
        put_row(array, TOP + 7, theirs)
        array[15:16, main] = array[7:8, main]
        array[8:9, main] = array[16:17, main]


def lag_pair(phase_lag, passage, half):
    count = phase_lag.shape[0]
    beside = lax.rem(passage + 2 * half - 1 + count, count)
    return phase_lag[passage, half], phase_lag[beside, 1 - half]


def relaxed(current, before, after, weights, forcing, width):
    sub = lax.broadcasted_iota(jnp.int32, (8, width), 0)
    inner = current[:, :width]
    below = jnp.where(sub == 0, pltpu.roll(before[:, :width], 1, 0), pltpu.roll(inner, 1, 0))
    above = jnp.where(sub == 7, pltpu.roll(after[:, :width], 7, 0), pltpu.roll(inner, 7, 0))
    left = pltpu.roll(current, 1, 1)[:, :width]
    right = pltpu.roll(current, WX - 1, 1)[:, :width]
    low = weights[0] * (below - inner) + weights[1] * (above - inner)
    side = weights[2] * (left - inner) + weights[3] * (right - inner)
    return (inner + forcing) + (low + side)


def step(source, target, weights, forcing, strip, rim, width, strips_too):
    def joined(own, edge):
        return own if width == W else jnp.concatenate([own, edge], axis=1)

    def one(start, row):
        own = pl.ds(row, 8)
        at = pl.ds(start, 8)
        w = [joined(weights[i, own, :], rim[i, at, :]) for i in range(4)]
        f = joined(forcing[own, :], rim[4, at, :])
        new = relaxed(
            source[at, :], source[pl.ds(start - 8, 8), :], source[pl.ds(start + 8, 8), :], w, f, width
        )
        return new

    def tile(t, carry):
        row = pl.multiple_of(8 * t, 8)
        start = pl.multiple_of(16 + 8 * t, 8)
        new = one(start, row)
        if target.shape[0] == ROWS:
            target[pl.ds(start, 8), :width] = new
        else:
            target[pl.ds(row, 8), :width] = new
        return carry

    lax.fori_loop(0, 32, tile, 0, unroll=2)
    if strips_too:
        for start, first, before, after in ((0, 0, 0, 8), (ROWS - 8, 8, ROWS - 16, ROWS - 8)):
            at = slice(start, start + 8)
            w = [joined(strip[i, first : first + 8, :], rim[i, at, :]) for i in range(4)]
            f = joined(strip[4, first : first + 8, :], rim[4, at, :])
            target[at, :width] = relaxed(
                source[at, :], source[before : before + 8, :], source[after : after + 8, :], w, f, width
            )


def strip_tiles(from_mid, from_plane, half, row, lanes):
    mid = from_mid[row : row + 8, lanes]
    plane = from_plane[row : row + 8, lanes]
    return jnp.where(half == 0, plane, mid), jnp.where(half == 0, mid, plane)


def packed_edge(block, sign):
    lane = lax.broadcasted_iota(jnp.int32, (PACKED, E), 1)
    spot = lane >> 3 if sign == 1 else 15 - (lane >> 3)
    out = jnp.zeros((PACKED, E), F32)
    for g in range(ROWS // PACKED):
        rows = block[PACKED * g : PACKED * (g + 1)]
        out = jnp.where(spot == g, pltpu.roll(rows, (sign * 8 * g) % E, 1) if g else rows, out)
    cell = lax.axis_index("cell")
    end = 0 if sign == 1 else lax.axis_size("cell") - 1
    return jnp.where(cell == end, 0.0, out)


def unpacked_edge(packed, sign):
    rows = [pltpu.roll(packed, (-sign * 8 * g) % E, 1) if g else packed for g in range(ROWS // PACKED)]
    return jnp.concatenate(rows, axis=0)


def edges_body(
    first, last, u_l, u_r, w_l, w_r, f_l, f_r, lagged, maps, from_mid, from_plane, phase_lag, to_left, to_right,
    array, own, other, wide,
):
    passage, half = place()
    full = slice(0, W)
    bottom, top = strip_tiles(from_mid, from_plane, half, 0, full)
    array[0:8, :] = bottom
    array[ROWS - 8 : ROWS, :] = top
    array[16:24, :] = first[...]
    array[TOP - 8 : TOP, :] = last[...]
    array[8:16, :] = jnp.zeros((8, W), F32)
    array[TOP : TOP + 8, :] = jnp.zeros((8, W), F32)
    keep_lagged(own, lagged.at[0])
    keep_lagged(other, from_plane.at[48:56])
    index = (square(maps[...]), square(from_plane[56:57, :]))
    fill_gaps(array, own, other, index, lag_pair(phase_lag, passage, half), half, 0)

    for out, block, u, w, f, sign in ((to_left, 0, u_l, w_l, f_l, 1), (to_right, 7, u_r, w_r, f_r, -1)):
        lanes = slice(128 * block, 128 * (block + 1))

        def packed(value, extra):
            lane = lax.broadcasted_iota(jnp.int32, value.shape, 1)
            for i, e in enumerate(extra):
                spot = 2 + i if sign == 1 else 125 - i
                value = jnp.where(lane == spot, pltpu.roll(e, (sign * (2 + i)) % 128, 1), value)
            return value

        wide[16:TOP, :] = packed(u[...], [w[0], w[1], w[2], w[3], f[...]])
        pairs = [strip_tiles(from_mid, from_plane, half, 8 * i, lanes) for i in range(6)]
        wide[0:8, :] = packed(pairs[0][0], [p[0] for p in pairs[1:]])
        wide[ROWS - 8 : ROWS, :] = packed(pairs[0][1], [p[1] for p in pairs[1:]])
        wide[8:16, :] = array[8:16, lanes]
        wide[TOP : TOP + 8, :] = array[TOP : TOP + 8, lanes]
        out[...] = packed_edge(wide[...], sign)


def edges(field, weights, forcing, lagged, maps, from_mid, from_plane, phase_lag):
    def spec(shape, *at):
        return pl.BlockSpec(shape, lambda i: at)

    whole = [spec((1, 8, W), 0, 0, 0), spec((1, W), 0, 0), spec((48, W), 0, 0), spec((64, W), 0, 0), smem()]
    return pl.pallas_call(
        edges_body,
        grid=(1,),
        out_shape=(EDGE,) * 2,
        in_specs=[
            spec((8, W), 0, 0),
            spec((8, W), 31, 0),
            spec((256, E), 0, 0),
            spec((256, E), 0, 7),
            spec((4, 256, E), 0, 0, 0),
            spec((4, 256, E), 0, 0, 7),
            spec((256, E), 0, 0),
            spec((256, E), 0, 7),
            *whole,
        ],
        out_specs=(spec((PACKED, E), 0, 0),) * 2,
        scratch_shapes=[
            pltpu.VMEM((ROWS, W), F32), pltpu.VMEM((16, 8, 128), F32), pltpu.VMEM((16, 8, 128), F32), pltpu.VMEM((ROWS, E), F32)
        ],
        compiler_params=params(),
        name="edges",
    )(field, field, field, field, weights, weights, forcing, forcing, lagged, maps, from_mid, from_plane, phase_lag)


def set_rim(array, left, right):
    lane = lax.broadcasted_iota(jnp.int32, (ROWS, E), 1)
    array[:, W:] = jnp.where(lane < 64, right, left)


def finish(level, source, between, out, surface, weights, forcing, strip, rim, own, other, index, lags, half, tail):
    step(source, between, weights, forcing, strip, rim, WX, True)
    surface[0:1, :] = between[16 + 128 : 17 + 128, :W]
    fill_gaps(between, own, other, index, lags, half, level + 1)
    step(between, out, weights, forcing, strip, rim, W, not tail)
    row = 128 if tail else 16 + 128
    surface[1:2, :] = out[row : row + 1, :]
    surface[2:8, :] = jnp.zeros((6, W), F32)


def first_body(
    field, weights, forcing, lagged, maps, from_mid, from_plane, from_left, from_right, phase_lag,
    out, to_left, to_right, surface, own, other, strip, rim, index, source, between,
):
    passage, half = place()
    full = slice(0, W)
    bottom, top = strip_tiles(from_mid, from_plane, half, 0, full)
    source[0:8, :W] = bottom
    source[ROWS - 8 : ROWS, :W] = top
    source[16:TOP, :W] = field[...]
    source[8:16, :W] = jnp.zeros((8, W), F32)
    source[TOP : TOP + 8, :W] = jnp.zeros((8, W), F32)
    left_edge, right_edge = unpacked_edge(from_left[...], -1), unpacked_edge(from_right[...], 1)
    set_rim(source, left_edge, right_edge)
    lane = lax.broadcasted_iota(jnp.int32, (ROWS, E), 1)
    for i in range(5):
        bottom, top = strip_tiles(from_mid, from_plane, half, 8 + 8 * i, full)
        strip[i, 0:8, :] = bottom
        strip[i, 8:16, :] = top
        right = pltpu.roll(right_edge, 128 - (2 + i), 1)
        left = pltpu.roll(left_edge, 2 + i, 1)
        rim[i, :, :] = jnp.where(lane == 0, right, jnp.where(lane == 127, left, 0.0))
    keep_lagged(own, lagged.at[0])
    keep_lagged(other, from_plane.at[48:56])
    own[8:16] = jnp.zeros((8, 8, 128), F32)
    other[8:16] = jnp.zeros((8, 8, 128), F32)
    index[0:8, :] = square(maps[...])
    index[8:16, :] = square(from_plane[56:57, :])
    pair = (index[0:8, :], index[8:16, :])
    lags = lag_pair(phase_lag, passage, half)
    fill_gaps(source, own, other, pair, lags, half, 0)
    out[8:16, :] = jnp.zeros((8, W), F32)
    out[TOP : TOP + 8, :] = jnp.zeros((8, W), F32)
    between[8:16, :] = jnp.zeros((8, WX), F32)
    between[TOP : TOP + 8, :] = jnp.zeros((8, WX), F32)
    finish(0, source, between, out, surface, weights, forcing, strip, rim, own, other, pair, lags, half, False)
    fill_gaps(out, own, other, pair, lags, half, 2)
    to_left[...] = packed_edge(out[:, :E], 1)
    to_right[...] = packed_edge(out[:, W - E :], -1)


def next_body(
    level, tail, state, weights, forcing, from_left, from_right, own_in, other_in, strip, rim, index, phase_lag, *rest
):
    if tail:
        out, surface, own, other, source, between = rest
    else:
        out, to_left, to_right, surface, own, other, source, between = rest
    passage, half = place()
    own[...] = own_in[...]
    other[...] = other_in[...]
    source[:, :W] = state[...]
    set_rim(source, unpacked_edge(from_left[...], -1), unpacked_edge(from_right[...], 1))
    between[8:16, :] = jnp.zeros((8, WX), F32)
    between[TOP : TOP + 8, :] = jnp.zeros((8, WX), F32)
    pair = (index[0:8, :], index[8:16, :])
    lags = lag_pair(phase_lag, passage, half)
    finish(level, source, between, out, surface, weights, forcing, strip, rim, own, other, pair, lags, half, tail)
    if not tail:
        out[8:16, :] = jnp.zeros((8, W), F32)
        out[TOP : TOP + 8, :] = jnp.zeros((8, W), F32)
        fill_gaps(out, own, other, pair, lags, half, level + 2)
        to_left[...] = packed_edge(out[:, :E], 1)
        to_right[...] = packed_edge(out[:, W - E :], -1)


HISTORY = jax.ShapeDtypeStruct((16, 8, 128), F32)
STATE = jax.ShapeDtypeStruct((ROWS, W), F32)
BUFFERS = [pltpu.VMEM((ROWS, WX), F32), pltpu.VMEM((ROWS, WX), F32)]
COST = pl.CostEstimate(flops=2 * 16 * 330 * 1024, bytes_accessed=8 << 20, transcendentals=0)


def first_steps(field, weights, forcing, lagged, maps, from_mid, from_plane, from_left, from_right, phase_lag):
    outs = (
        STATE, EDGE, EDGE, jax.ShapeDtypeStruct((8, W), F32), HISTORY, HISTORY,
        jax.ShapeDtypeStruct((5, 16, W), F32), jax.ShapeDtypeStruct((5, ROWS, E), F32),
        jax.ShapeDtypeStruct((16, 128), jnp.int32),
    )
    return pl.pallas_call(
        first_body,
        out_shape=outs,
        in_specs=[vmem()] * 9 + [smem()],
        out_specs=tuple(vmem() for _ in outs),
        scratch_shapes=BUFFERS,
        compiler_params=params(),
        cost_estimate=COST,
        name="steps_first",
    )(field, weights, forcing, lagged, maps, from_mid, from_plane, from_left, from_right, phase_lag)


def next_steps(level, state, weights, forcing, from_left, from_right, own, other, strip, rim, index, phase_lag):
    tail = level == STEPS - 2
    surface = jax.ShapeDtypeStruct((8, W), F32)
    if tail:
        outs = (jax.ShapeDtypeStruct((256, W), F32), surface)
        scratch = [pltpu.VMEM((16, 8, 128), F32), pltpu.VMEM((16, 8, 128), F32), *BUFFERS]
    else:
        outs = (STATE, EDGE, EDGE, surface, HISTORY, HISTORY)
        scratch = BUFFERS
    return pl.pallas_call(
        functools.partial(next_body, level, tail),
        out_shape=outs,
        in_specs=[vmem()] * 10 + [smem()],
        out_specs=tuple(vmem() for _ in outs),
        scratch_shapes=scratch,
        compiler_params=params(),
        cost_estimate=COST,
        name=f"steps_{level}",
    )(state, weights, forcing, from_left, from_right, own, other, strip, rim, index, phase_lag)


def kernels_body(points, radius, angle, axial, stagger, area, press, change, *, scale, passages):
    passage, half = place()

    def mine(ref):
        return jnp.where(half == 0, ref[0:1, :], ref[1:2, :])

    phase = passage.astype(F32) * (2.0 * math.pi / passages) + mine(angle)
    cos_phase, sin_phase = jnp.cos(phase), jnp.sin(phase)
    cos_stagger = jnp.cos(mine(stagger))
    weight = mine(area) * (scale / (4.0 * math.pi))
    normal_x = -weight * cos_stagger * sin_phase
    normal_y = weight * cos_stagger * cos_phase
    normal_z = weight * jnp.sin(mine(stagger))
    face_x = mine(radius) * cos_phase
    face_y = mine(radius) * sin_phase
    face_z = mine(axial)

    def tile(t, carry):
        rows = pl.ds(pl.multiple_of(16 * t, 16), 16)
        at = points[rows, :]
        delta_x = at[:, 0:1] - face_x
        delta_y = at[:, 1:2] - face_y
        delta_z = at[:, 2:3] - face_z
        inverse = lax.rsqrt(delta_x * delta_x + delta_y * delta_y + delta_z * delta_z)
        along = normal_x * delta_x + normal_y * delta_y + normal_z * delta_z
        both = along * inverse * inverse
        press[rows, :] = (both * inverse).astype(jnp.bfloat16)
        change[rows, :] = (both * (1.0 / sound_speed)).astype(jnp.bfloat16)
        return carry

    lax.fori_loop(0, press.shape[0] // 16, tile, 0)


def kernels(points, radius, angle, axial, stagger, area, part, count, scale, passages):
    size = points.shape[0] // count
    faces = pl.BlockSpec((2, W), lambda i: (0, 0))
    shape = jax.ShapeDtypeStruct((size, W), jnp.bfloat16)
    return pl.pallas_call(
        functools.partial(kernels_body, scale=scale, passages=passages),
        grid=(1,),
        out_shape=(shape, shape),
        in_specs=[pl.BlockSpec((size, 3), lambda i: (part, 0))] + [faces] * 5,
        out_specs=(pl.BlockSpec((size, W), lambda i: (0, 0)),) * 2,
        compiler_params=params(),
        cost_estimate=pl.CostEstimate(flops=20 * size * W, bytes_accessed=4 * size * W, transcendentals=size * W),
        name=f"kernels_{part}",
    )(points, radius, angle, axial, stagger, area)


def sound_body(*refs):
    presses, changes, (record, s0, s1, s2, s3, group, out, total) = refs[:4], refs[4:8], refs[8:]
    late = jnp.concatenate([s[0:2, :] for s in (s0, s1, s2, s3)], axis=0).astype(jnp.bfloat16)
    surface = jnp.concatenate([record[0].astype(F32), late.astype(F32)], axis=0)
    times = surface.shape[0]
    row = lax.broadcasted_iota(jnp.int32, surface.shape, 0)
    after, before = pltpu.roll(surface, times - 1, 0), pltpu.roll(surface, 1, 0)
    first = row == 0
    last = row == times - 1
    rate = jnp.where(last, surface, after) - jnp.where(first, surface, before)
    rate = jnp.where(first | last, rate, rate * 0.5).astype(jnp.bfloat16)
    surface = surface.astype(jnp.bfloat16)
    turned = (((1,), (1,)), ((), ()))
    size = presses[0].shape[0]
    for n in range(4):
        got = lax.dot_general(presses[n][...], surface, turned, preferred_element_type=F32)
        got = got + lax.dot_general(changes[n][...], rate, turned, preferred_element_type=F32)
        total[size * n : size * (n + 1), :] = got
    label = lax.broadcasted_iota(jnp.int32, (GROUPS, group.shape[1]), 0)
    member = (group[...] == label).astype(F32)
    counts = jnp.sum(member, axis=1, keepdims=True)
    means = jnp.dot(member, total[...], precision=lax.Precision.HIGHEST, preferred_element_type=F32)
    means = means / jnp.maximum(counts, 1.0)
    for s in range(8):
        for c in range(4):
            start = 256 * c + 32 * s
            out[4 * s + c, 0:32, :] = total[start : start + 32, :]
            out[4 * s + c, 32:34, :] = means[2 * s : 2 * s + 2, :]
            out[4 * s + c, 34:40, :] = jnp.zeros((6, 128), F32)


def sound(presses, changes, record, surfaces, group):
    return pl.pallas_call(
        sound_body,
        out_shape=jax.ShapeDtypeStruct((32, 40, 128), F32),
        in_specs=[vmem()] * 14,
        out_specs=vmem(),
        scratch_shapes=[pltpu.VMEM((1024, 128), F32)],
        compiler_params=params(),
        name="sound",
    )(*presses, *changes, record, *surfaces, group)


def exchanged(pieces, axes):
    return lax.all_to_all(pieces, axes, 0, 0, tiled=True)


def sent_to_all(block, axes):
    count = lax.axis_size(axes)
    return exchanged(jnp.broadcast_to(block, (count, *block.shape)), axes)


def on_device(
    flow_state,
    face_weights,
    forcing,
    lagged_planes,
    phase_lag,
    face_map,
    surface_record,
    face_radius,
    face_angle,
    face_axial,
    face_stagger,
    face_area,
    listeners,
    observer_group,
):
    passes = lax.axis_size(PASS)
    cells = lax.axis_size("cell")
    scale = 64.0 / math.sqrt(W * cells * passes)
    across = [(i, i ^ 1) for i in range(passes)]
    over = [(i, ((i + 1) ^ 1) - 1 if 0 < i < passes - 1 else passes - 1 - i) for i in range(passes)]
    rightward = [(i, (i + 1) % cells) for i in range(cells)]
    leftward = [(j, i) for i, j in rightward]

    far = (flow_state, face_weights, forcing, lagged_planes)
    to_mid, to_plane = strips(*[pltpu.with_memory_space_constraint(x, pltpu.HBM) for x in far], face_map)
    points, to_mid, to_plane, far = lax.optimization_barrier((listeners.T, to_mid, to_plane, far[:3]))
    from_mid = lax.ppermute(to_mid, PASS, across)
    from_plane = lax.ppermute(to_plane, PASS, over)

    pairs = [
        kernels(points, face_radius, face_angle, face_axial, face_stagger, face_area, n, 4, scale, passes // 2)
        for n in range(4)
    ]

    near = load([pltpu.with_memory_space_constraint(x, pltpu.HBM) for x in far])
    pairs, near, from_mid, from_plane = lax.optimization_barrier((pairs, near, from_mid, from_plane))
    flow_state, face_weights, forcing = [pltpu.with_memory_space_constraint(x, pltpu.VMEM) for x in near]
    to_left, to_right = edges(
        flow_state, face_weights, forcing, lagged_planes, face_map, from_mid, from_plane, phase_lag
    )
    from_left = lax.ppermute(to_right, "cell", rightward)
    from_right = lax.ppermute(to_left, "cell", leftward)
    state, to_left, to_right, surface, own, other, strip, rim, index = first_steps(
        flow_state, face_weights, forcing, lagged_planes, face_map, from_mid, from_plane, from_left, from_right,
        phase_lag,
    )
    surfaces = [surface]
    for level in range(2, STEPS, 2):
        from_left = lax.ppermute(to_right, "cell", rightward)
        from_right = lax.ppermute(to_left, "cell", leftward)
        got = next_steps(
            level, state, face_weights, forcing, from_left, from_right, own, other, strip, rim, index, phase_lag
        )
        if level < STEPS - 2:
            state, to_left, to_right, surface, own, other = got
        else:
            state, surface = got
        surfaces.append(surface)

    pieces = sound(
        [p[0] for p in pairs], [p[1] for p in pairs], surface_record, surfaces, observer_group[None, :]
    )
    part = jnp.sum(exchanged(pieces, ("x", "y_hi", "cell")), axis=0)
    part = jnp.sum(sent_to_all(part, "z"), axis=0)
    parts = sent_to_all(part, ("x", "y_hi"))
    acoustic = parts[:, :32].reshape(256, 128)
    array_signal = parts[:, 32:34].reshape(GROUPS, 128)
    return state, acoustic, array_signal


def solution(mesh):
    sizes = tuple(SPLIT.values())
    fine = Mesh(mesh.devices.reshape(*sizes, mesh.shape["cell"]), (*PASS, "cell"))
    return jax.shard_map(
        on_device,
        mesh=fine,
        in_specs=(
            P(PASS, "cell"),
            P(None, PASS, "cell"),
            P(PASS, "cell"),
            P(PASS, None, "cell"),
            P(),
            P(PASS, "cell"),
            P(PASS, None, "cell"),
            P(None, "cell"),
            P(None, "cell"),
            P(None, "cell"),
            P(None, "cell"),
            P(None, "cell"),
            P(),
            P(),
        ),
        out_specs=(P(PASS, "cell"), P("cell", None), P()),
        check_vma=False,
    )
```

```python
import functools
import math

import jax
import jax.numpy as jnp
from jax import lax
from jax.experimental import pallas as pl
from jax.experimental.pallas import tpu as pltpu
from jax.sharding import Mesh
from jax.sharding import PartitionSpec as P

STEPS = 8
GROUPS = 16
sound_speed = 2.0

W = 1024
E = 128
WX = W + E
TOP = 16 + 256
ROWS = TOP + 16
PACKED = 24
SPLIT = {"x": 4, "z": 8, "y_hi": 2}
PASS = ("x", "z", "y_hi")
VMEM_LIMIT = 8 * 1024 * 1024
F32 = jnp.float32
EDGE = jax.ShapeDtypeStruct((PACKED, E), F32)
HISTORY = jax.ShapeDtypeStruct((16, 8, 128), F32)
INDEX = jax.ShapeDtypeStruct((32, 128), jnp.int32)
GAPS = jax.ShapeDtypeStruct((16, W), F32)


def params(**kw):
    return pltpu.CompilerParams(vmem_limit_bytes=VMEM_LIMIT, **kw)


def vmem():
    return pl.BlockSpec(memory_space=pltpu.VMEM)


def place():
    index = lax.axis_index("x") * (SPLIT["z"] * SPLIT["y_hi"]) + lax.axis_index("z") * SPLIT["y_hi"]
    index = index + lax.axis_index("y_hi")
    return index // 2, index % 2


def strips_body(field, weights, forcing, lagged, maps, to_mid, to_plane, row, sems):
    _, half = place()
    mid = pl.multiple_of(jnp.where(half == 0, 248, 0), 8)
    plane = pl.multiple_of(jnp.where(half == 0, 0, 248), 8)
    copies = []
    for out, start in ((to_mid, mid), (to_plane, plane)):
        rows = pl.ds(start, 8)
        copies.append((field.at[rows], out.at[pl.ds(0, 8)]))
        for i in range(4):
            copies.append((weights.at[i, rows], out.at[pl.ds(8 + 8 * i, 8)]))
        copies.append((forcing.at[rows], out.at[pl.ds(40, 8)]))
    copies.append((lagged.at[0], to_plane.at[pl.ds(48, 8)]))
    copies.append((maps, row))
    started = []
    for n, (source, target) in enumerate(copies):
        copy = pltpu.make_async_copy(source, target, sems.at[n])
        copy.start()
        started.append(copy)
    for copy in started:
        copy.wait()
    to_plane[56:64, :] = jnp.broadcast_to(row[...].astype(F32), (8, W))


def strips(field, weights, forcing, lagged, maps):
    anywhere = pl.BlockSpec(memory_space=pltpu.HBM)
    return pl.pallas_call(
        strips_body,
        out_shape=(jax.ShapeDtypeStruct((48, W), F32), jax.ShapeDtypeStruct((64, W), F32)),
        in_specs=[anywhere] * 5,
        out_specs=(vmem(), vmem()),
        scratch_shapes=[pltpu.VMEM((1, W), jnp.int32), pltpu.SemaphoreType.DMA((14,))],
        compiler_params=params(),
        name="strips",
    )(field, weights, forcing, lagged, maps)


def load_body(*refs):
    count = (len(refs) - 1) // 2
    copies = [pltpu.make_async_copy(refs[n], refs[count + n], refs[-1].at[n]) for n in range(count)]
    for copy in copies:
        copy.start()
    for copy in copies:
        copy.wait()


def load(arrays):
    count = len(arrays)
    return pl.pallas_call(
        load_body,
        out_shape=tuple(jax.ShapeDtypeStruct(a.shape, a.dtype) for a in arrays),
        in_specs=[pl.BlockSpec(memory_space=pltpu.HBM)] * count,
        out_specs=(vmem(),) * count,
        scratch_shapes=[pltpu.SemaphoreType.DMA((count,))],
        compiler_params=params(),
        cost_estimate=pl.CostEstimate(flops=0, bytes_accessed=12 << 20, transcendentals=0),
        name="load",
    )(*arrays)


def square(row):
    tiles = [row[:, 128 * s : 128 * (s + 1)] for s in range(8)]
    return jnp.concatenate(tiles, axis=0).astype(jnp.int32) & (W - 1)


def picked(history, level, lag, index):
    back = level - lag
    row = jnp.where(back >= 0, 8 + back, -back - 1)
    tiles = history[0]
    for n in range(1, 9 + level):
        tiles = jnp.where(row == n, history[n], tiles)
    high, low = index >> 7, index & 127
    out = jnp.zeros((8, 128), F32)
    for b in range(8):
        source = jnp.broadcast_to(tiles[b : b + 1, :], (8, 128))
        value = jnp.take_along_axis(source, low, axis=1, mode="promise_in_bounds")
        out = jnp.where(high == b, value, out)
    return out


def keep_lagged(history, lagged):
    for j in range(8):
        for b in range(8):
            history[j, b : b + 1, :] = lagged[j : j + 1, 128 * b : 128 * (b + 1)]


def fill_gaps(array, own, other, index, half, level):
    low = half == 0
    lanes = [slice(128 * b, 128 * (b + 1)) for b in range(8)]
    ends = [[array[r : r + 1, k] for k in lanes] for r in (7, 16, TOP - 1, TOP + 8)]
    for b in range(8):
        own[8 + level, b : b + 1, :] = jnp.where(low, ends[1][b], ends[2][b])
        other[8 + level, b : b + 1, :] = jnp.where(low, ends[0][b], ends[3][b])
    mine = picked(other, level, index[16:24, :], index[0:8, :])
    theirs = picked(own, level, index[24:32, :], index[8:16, :])
    for b, k in enumerate(lanes):
        array[15:16, k] = jnp.where(low, mine[b : b + 1], ends[0][b])
        array[8:9, k] = jnp.where(low, theirs[b : b + 1], ends[1][b])
        array[TOP : TOP + 1, k] = jnp.where(low, ends[3][b], mine[b : b + 1])
        array[TOP + 7 : TOP + 8, k] = jnp.where(low, ends[2][b], theirs[b : b + 1])


def lag_square(phase_lag, row, column):
    count, sides = phase_lag.shape
    at = lax.broadcasted_iota(jnp.int32, (count, sides), 0) == row
    at = at & (lax.broadcasted_iota(jnp.int32, (count, sides), 1) == column)
    lag = jnp.sum(jnp.where(at, phase_lag[...].astype(F32), 0.0), axis=0, keepdims=True)
    lag = jnp.sum(lag, axis=1, keepdims=True)
    return jnp.broadcast_to(lag, (8, 128)).astype(jnp.int32)


def set_index(index, maps, other_maps, phase_lag, passage, half):
    count = phase_lag.shape[0]
    index[0:8, :] = square(maps)
    index[8:16, :] = square(other_maps)
    index[16:24, :] = lag_square(phase_lag, passage, half)
    index[24:32, :] = lag_square(phase_lag, lax.rem(passage + 2 * half - 1 + count, count), 1 - half)


def relaxed(current, before, after, weights, forcing, width):
    sub = lax.broadcasted_iota(jnp.int32, (8, width), 0)
    inner = current[:, :width]
    below = jnp.where(sub == 0, pltpu.roll(before[:, :width], 1, 0), pltpu.roll(inner, 1, 0))
    above = jnp.where(sub == 7, pltpu.roll(after[:, :width], 7, 0), pltpu.roll(inner, 7, 0))
    left = pltpu.roll(current, 1, 1)[:, :width]
    right = pltpu.roll(current, WX - 1, 1)[:, :width]
    low = weights[0] * (below - inner) + weights[1] * (above - inner)
    side = weights[2] * (left - inner) + weights[3] * (right - inner)
    return (inner + forcing) + (low + side)


def step(source, target, weights, forcing, strip, rim, width, strips_too):
    def joined(own, edge):
        return own if width == W else jnp.concatenate([own, edge], axis=1)

    def one(start, row):
        own = pl.ds(row, 8)
        at = pl.ds(start, 8)
        w = [joined(weights[i, own, :], rim[i, at, :]) for i in range(4)]
        f = joined(forcing[own, :], rim[4, at, :])
        new = relaxed(
            source[at, :], source[pl.ds(start - 8, 8), :], source[pl.ds(start + 8, 8), :], w, f, width
        )
        return new

    def tile(t, carry):
        row = pl.multiple_of(8 * t, 8)
        start = pl.multiple_of(16 + 8 * t, 8)
        new = one(start, row)
        if target.shape[0] == ROWS:
            target[pl.ds(start, 8), :width] = new
        else:
            target[pl.ds(row, 8), :width] = new
        return carry

    lax.fori_loop(0, 32, tile, 0, unroll=True)
    if strips_too:
        for start, first, before, after in ((0, 0, 0, 8), (ROWS - 8, 8, ROWS - 16, ROWS - 8)):
            at = slice(start, start + 8)
            w = [joined(strip[i, first : first + 8, :], rim[i, at, :]) for i in range(4)]
            f = joined(strip[4, first : first + 8, :], rim[4, at, :])
            target[at, :width] = relaxed(
                source[at, :], source[before : before + 8, :], source[after : after + 8, :], w, f, width
            )


def strip_tiles(from_mid, from_plane, half, row, lanes):
    mid = from_mid[row : row + 8, lanes]
    plane = from_plane[row : row + 8, lanes]
    return jnp.where(half == 0, plane, mid), jnp.where(half == 0, mid, plane)


def packed_edge(block, sign):
    lane = lax.broadcasted_iota(jnp.int32, (PACKED, E), 1)
    spot = lane >> 3 if sign == 1 else 15 - (lane >> 3)
    out = jnp.zeros((PACKED, E), F32)
    for g in range(ROWS // PACKED):
        rows = block[PACKED * g : PACKED * (g + 1)]
        out = jnp.where(spot == g, pltpu.roll(rows, (sign * 8 * g) % E, 1) if g else rows, out)
    cell = lax.axis_index("cell")
    end = 0 if sign == 1 else lax.axis_size("cell") - 1
    return jnp.where(cell == end, 0.0, out)


def unpacked_edge(packed, sign):
    rows = [pltpu.roll(packed, (-sign * 8 * g) % E, 1) if g else packed for g in range(ROWS // PACKED)]
    return jnp.concatenate(rows, axis=0)


def edges_body(
    first, last, u_l, u_r, w_l, w_r, f_l, f_r, lagged, maps, from_mid, from_plane, phase_lag, to_left, to_right,
    own, other, index, gaps, array, wide,
):
    passage, half = place()
    full = slice(0, W)
    bottom, top = strip_tiles(from_mid, from_plane, half, 0, full)
    array[0:8, :] = bottom
    array[ROWS - 8 : ROWS, :] = top
    array[16:24, :] = first[...]
    array[TOP - 8 : TOP, :] = last[...]
    array[8:16, :] = jnp.zeros((8, W), F32)
    array[TOP : TOP + 8, :] = jnp.zeros((8, W), F32)
    keep_lagged(own, lagged.at[0])
    keep_lagged(other, from_plane.at[48:56])
    own[8:16] = jnp.zeros((8, 8, 128), F32)
    other[8:16] = jnp.zeros((8, 8, 128), F32)
    set_index(index, maps[...], from_plane[56:57, :], phase_lag, passage, half)
    fill_gaps(array, own, other, index, half, 0)
    gaps[0:8, :] = array[8:16, :]
    gaps[8:16, :] = array[TOP : TOP + 8, :]

    for out, block, u, w, f, sign in ((to_left, 0, u_l, w_l, f_l, 1), (to_right, 7, u_r, w_r, f_r, -1)):
        lanes = slice(128 * block, 128 * (block + 1))

        def packed(value, extra):
            lane = lax.broadcasted_iota(jnp.int32, value.shape, 1)
            for i, e in enumerate(extra):
                spot = 2 + i if sign == 1 else 125 - i
                value = jnp.where(lane == spot, pltpu.roll(e, (sign * (2 + i)) % 128, 1), value)
            return value

        wide[16:TOP, :] = packed(u[...], [w[0], w[1], w[2], w[3], f[...]])
        pairs = [strip_tiles(from_mid, from_plane, half, 8 * i, lanes) for i in range(6)]
        wide[0:8, :] = packed(pairs[0][0], [p[0] for p in pairs[1:]])
        wide[ROWS - 8 : ROWS, :] = packed(pairs[0][1], [p[1] for p in pairs[1:]])
        wide[8:16, :] = array[8:16, lanes]
        wide[TOP : TOP + 8, :] = array[TOP : TOP + 8, lanes]
        out[...] = packed_edge(wide[...], sign)


def edges(field, weights, forcing, lagged, maps, from_mid, from_plane, phase_lag):
    def spec(shape, *at):
        return pl.BlockSpec(shape, lambda i: at)

    whole = [spec((1, 8, W), 0, 0, 0), spec((1, W), 0, 0), spec((48, W), 0, 0), spec((64, W), 0, 0), spec((32, 2), 0, 0)]
    return pl.pallas_call(
        edges_body,
        grid=(1,),
        out_shape=(EDGE, EDGE, HISTORY, HISTORY, INDEX, GAPS),
        in_specs=[
            spec((8, W), 0, 0),
            spec((8, W), 31, 0),
            spec((256, E), 0, 0),
            spec((256, E), 0, 7),
            spec((4, 256, E), 0, 0, 0),
            spec((4, 256, E), 0, 0, 7),
            spec((256, E), 0, 0),
            spec((256, E), 0, 7),
            *whole,
        ],
        out_specs=(
            spec((PACKED, E), 0, 0), spec((PACKED, E), 0, 0), spec((16, 8, 128), 0, 0, 0), spec((16, 8, 128), 0, 0, 0),
            spec((32, 128), 0, 0), spec((16, W), 0, 0),
        ),
        scratch_shapes=[pltpu.VMEM((ROWS, W), F32), pltpu.VMEM((ROWS, E), F32)],
        compiler_params=params(),
        name="edges",
    )(field, field, field, field, weights, weights, forcing, forcing, lagged, maps, from_mid, from_plane, phase_lag)


def set_rim(array, left, right):
    lane = lax.broadcasted_iota(jnp.int32, (ROWS, E), 1)
    array[:, W:] = jnp.where(lane < 64, right, left)


def finish(level, source, between, out, surface, weights, forcing, strip, rim, own, other, index, half, tail):
    step(source, between, weights, forcing, strip, rim, WX, True)
    surface[0:1, :] = between[16 + 128 : 17 + 128, :W]
    fill_gaps(between, own, other, index, half, level + 1)
    step(between, out, weights, forcing, strip, rim, W, not tail)
    row = 128 if tail else 16 + 128
    surface[1:2, :] = out[row : row + 1, :]
    surface[2:8, :] = jnp.zeros((6, W), F32)


def first_body(
    field, weights, forcing, gaps, from_mid, from_plane, from_left, from_right, own_in, other_in, index,
    out, to_left, to_right, surface, own, other, strip, rim, source, between,
):
    _, half = place()
    full = slice(0, W)
    bottom, top = strip_tiles(from_mid, from_plane, half, 0, full)
    source[0:8, :W] = bottom
    source[ROWS - 8 : ROWS, :W] = top
    source[16:TOP, :W] = field[...]
    source[8:16, :W] = gaps[0:8, :]
    source[TOP : TOP + 8, :W] = gaps[8:16, :]
    left_edge, right_edge = unpacked_edge(from_left[...], -1), unpacked_edge(from_right[...], 1)
    set_rim(source, left_edge, right_edge)
    lane = lax.broadcasted_iota(jnp.int32, (ROWS, E), 1)
    for i in range(5):
        bottom, top = strip_tiles(from_mid, from_plane, half, 8 + 8 * i, full)
        strip[i, 0:8, :] = bottom
        strip[i, 8:16, :] = top
        right = pltpu.roll(right_edge, 128 - (2 + i), 1)
        left = pltpu.roll(left_edge, 2 + i, 1)
        rim[i, :, :] = jnp.where(lane == 0, right, jnp.where(lane == 127, left, 0.0))
    own[...] = own_in[...]
    other[...] = other_in[...]
    out[8:16, :] = jnp.zeros((8, W), F32)
    out[TOP : TOP + 8, :] = jnp.zeros((8, W), F32)
    between[8:16, :] = jnp.zeros((8, WX), F32)
    between[TOP : TOP + 8, :] = jnp.zeros((8, WX), F32)
    finish(0, source, between, out, surface, weights, forcing, strip, rim, own, other, index, half, False)
    fill_gaps(out, own, other, index, half, 2)
    to_left[...] = packed_edge(out[:, :E], 1)
    to_right[...] = packed_edge(out[:, W - E :], -1)


def next_body(
    level, tail, state, weights, forcing, from_left, from_right, own_in, other_in, strip, rim, index, *rest
):
    if tail:
        out, surface, own, other, source, between = rest
    else:
        out, to_left, to_right, surface, own, other, source, between = rest
    _, half = place()
    own[...] = own_in[...]
    other[...] = other_in[...]
    source[:, :W] = state[...]
    set_rim(source, unpacked_edge(from_left[...], -1), unpacked_edge(from_right[...], 1))
    between[8:16, :] = jnp.zeros((8, WX), F32)
    between[TOP : TOP + 8, :] = jnp.zeros((8, WX), F32)
    finish(level, source, between, out, surface, weights, forcing, strip, rim, own, other, index, half, tail)
    if not tail:
        out[8:16, :] = jnp.zeros((8, W), F32)
        out[TOP : TOP + 8, :] = jnp.zeros((8, W), F32)
        fill_gaps(out, own, other, index, half, level + 2)
        to_left[...] = packed_edge(out[:, :E], 1)
        to_right[...] = packed_edge(out[:, W - E :], -1)


STATE = jax.ShapeDtypeStruct((ROWS, W), F32)
BUFFERS = [pltpu.VMEM((ROWS, WX), F32), pltpu.VMEM((ROWS, WX), F32)]
COST = pl.CostEstimate(flops=2 * 16 * 330 * 1024, bytes_accessed=8 << 20, transcendentals=0)


def first_steps(field, weights, forcing, gaps, from_mid, from_plane, from_left, from_right, own, other, index):
    outs = (
        STATE, EDGE, EDGE, jax.ShapeDtypeStruct((8, W), F32), HISTORY, HISTORY,
        jax.ShapeDtypeStruct((5, 16, W), F32), jax.ShapeDtypeStruct((5, ROWS, E), F32),
    )
    return pl.pallas_call(
        first_body,
        out_shape=outs,
        in_specs=[vmem()] * 11,
        out_specs=tuple(vmem() for _ in outs),
        scratch_shapes=BUFFERS,
        compiler_params=params(),
        cost_estimate=COST,
        name="steps_first",
    )(field, weights, forcing, gaps, from_mid, from_plane, from_left, from_right, own, other, index)


def next_steps(level, state, weights, forcing, from_left, from_right, own, other, strip, rim, index):
    tail = level == STEPS - 2
    surface = jax.ShapeDtypeStruct((8, W), F32)
    if tail:
        outs = (jax.ShapeDtypeStruct((256, W), F32), surface)
        scratch = [pltpu.VMEM((16, 8, 128), F32), pltpu.VMEM((16, 8, 128), F32), *BUFFERS]
    else:
        outs = (STATE, EDGE, EDGE, surface, HISTORY, HISTORY)
        scratch = BUFFERS
    return pl.pallas_call(
        functools.partial(next_body, level, tail),
        out_shape=outs,
        in_specs=[vmem()] * 10,
        out_specs=tuple(vmem() for _ in outs),
        scratch_shapes=scratch,
        compiler_params=params(),
        cost_estimate=COST,
        name=f"steps_{level}",
    )(state, weights, forcing, from_left, from_right, own, other, strip, rim, index)


def kernels_body(points, radius, angle, axial, stagger, area, press, change, *, scale, passages):
    passage, half = place()

    def mine(ref):
        return jnp.where(half == 0, ref[0:1, :], ref[1:2, :])

    phase = passage.astype(F32) * (2.0 * math.pi / passages) + mine(angle)
    cos_phase, sin_phase = jnp.cos(phase), jnp.sin(phase)
    cos_stagger = jnp.cos(mine(stagger))
    weight = mine(area) * (scale / (4.0 * math.pi))
    normal_x = -weight * cos_stagger * sin_phase
    normal_y = weight * cos_stagger * cos_phase
    normal_z = weight * jnp.sin(mine(stagger))
    face_x = mine(radius) * cos_phase
    face_y = mine(radius) * sin_phase
    face_z = mine(axial)

    def tile(t, carry):
        rows = pl.ds(pl.multiple_of(16 * t, 16), 16)
        at = points[rows, :]
        delta_x = at[:, 0:1] - face_x
        delta_y = at[:, 1:2] - face_y
        delta_z = at[:, 2:3] - face_z
        inverse = lax.rsqrt(delta_x * delta_x + delta_y * delta_y + delta_z * delta_z)
        along = normal_x * delta_x + normal_y * delta_y + normal_z * delta_z
        both = along * inverse * inverse
        press[rows, :] = (both * inverse).astype(jnp.bfloat16)
        change[rows, :] = (both * (1.0 / sound_speed)).astype(jnp.bfloat16)
        return carry

    lax.fori_loop(0, press.shape[0] // 16, tile, 0, unroll=True)


def kernels(points, radius, angle, axial, stagger, area, part, count, scale, passages):
    size = points.shape[0] // count
    faces = pl.BlockSpec((2, W), lambda i: (0, 0))
    shape = jax.ShapeDtypeStruct((size, W), jnp.bfloat16)
    return pl.pallas_call(
        functools.partial(kernels_body, scale=scale, passages=passages),
        grid=(1,),
        out_shape=(shape, shape),
        in_specs=[pl.BlockSpec((size, 3), lambda i: (part, 0))] + [faces] * 5,
        out_specs=(pl.BlockSpec((size, W), lambda i: (0, 0)),) * 2,
        compiler_params=params(),
        cost_estimate=pl.CostEstimate(flops=20 * size * W, bytes_accessed=4 * size * W, transcendentals=size * W),
        name=f"kernels_{part}",
    )(points, radius, angle, axial, stagger, area)


def sound_body(*refs):
    presses, changes, (record, s0, s1, s2, s3, group, out, total) = refs[:4], refs[4:8], refs[8:]
    late = jnp.concatenate([s[0:2, :] for s in (s0, s1, s2, s3)], axis=0).astype(jnp.bfloat16)
    surface = jnp.concatenate([record[0].astype(F32), late.astype(F32)], axis=0)
    times = surface.shape[0]
    row = lax.broadcasted_iota(jnp.int32, surface.shape, 0)
    after, before = pltpu.roll(surface, times - 1, 0), pltpu.roll(surface, 1, 0)
    first = row == 0
    last = row == times - 1
    rate = jnp.where(last, surface, after) - jnp.where(first, surface, before)
    rate = jnp.where(first | last, rate, rate * 0.5).astype(jnp.bfloat16)
    surface = surface.astype(jnp.bfloat16)
    turned = (((1,), (1,)), ((), ()))
    size = presses[0].shape[0]
    for n in range(4):
        got = lax.dot_general(presses[n][...], surface, turned, preferred_element_type=F32)
        got = got + lax.dot_general(changes[n][...], rate, turned, preferred_element_type=F32)
        total[size * n : size * (n + 1), :] = got
    label = lax.broadcasted_iota(jnp.int32, (GROUPS, group.shape[1]), 0)
    member = (group[...] == label).astype(F32)
    counts = jnp.sum(member, axis=1, keepdims=True)
    means = jnp.dot(member, total[...], precision=lax.Precision.HIGHEST, preferred_element_type=F32)
    means = means / jnp.maximum(counts, 1.0)
    for s in range(8):
        for c in range(4):
            start = 256 * c + 32 * s
            out[4 * s + c, 0:32, :] = total[start : start + 32, :]
            out[4 * s + c, 32:34, :] = means[2 * s : 2 * s + 2, :]
            out[4 * s + c, 34:40, :] = jnp.zeros((6, 128), F32)


def sound(presses, changes, record, surfaces, group):
    return pl.pallas_call(
        sound_body,
        out_shape=jax.ShapeDtypeStruct((32, 40, 128), F32),
        in_specs=[vmem()] * 14,
        out_specs=vmem(),
        scratch_shapes=[pltpu.VMEM((1024, 128), F32)],
        compiler_params=params(),
        name="sound",
    )(*presses, *changes, record, *surfaces, group)


def placed_body(parts, acoustic, array_signal):
    for s in range(8):
        acoustic[32 * s : 32 * (s + 1), :] = parts[s, 0:32, :]
        array_signal[2 * s : 2 * s + 2, :] = parts[s, 32:34, :]


def placed(parts):
    return pl.pallas_call(
        placed_body,
        out_shape=(jax.ShapeDtypeStruct((256, 128), F32), jax.ShapeDtypeStruct((GROUPS, 128), F32)),
        in_specs=[vmem()],
        out_specs=(vmem(), vmem()),
        compiler_params=params(),
        name="placed",
    )(parts)


def exchanged(pieces, axes):
    return lax.all_to_all(pieces, axes, 0, 0, tiled=True)


def sent_to_all(block, axes):
    count = lax.axis_size(axes)
    return exchanged(jnp.broadcast_to(block, (count, *block.shape)), axes)


def on_device(
    flow_state,
    face_weights,
    forcing,
    lagged_planes,
    phase_lag,
    face_map,
    surface_record,
    face_radius,
    face_angle,
    face_axial,
    face_stagger,
    face_area,
    listeners,
    observer_group,
):
    passes = lax.axis_size(PASS)
    cells = lax.axis_size("cell")
    scale = 64.0 / math.sqrt(W * cells * passes)
    across = [(i, i ^ 1) for i in range(passes)]
    over = [(i, ((i + 1) ^ 1) - 1 if 0 < i < passes - 1 else passes - 1 - i) for i in range(passes)]
    rightward = [(i, (i + 1) % cells) for i in range(cells)]
    leftward = [(j, i) for i, j in rightward]

    far = (flow_state, face_weights, forcing, lagged_planes, face_map)
    to_mid, to_plane = strips(*[pltpu.with_memory_space_constraint(x, pltpu.HBM) for x in far])
    listeners, to_mid, to_plane, far = lax.optimization_barrier((listeners, to_mid, to_plane, far[:3]))
    points = listeners.T
    from_mid = lax.ppermute(to_mid, PASS, across)
    from_plane = lax.ppermute(to_plane, PASS, over)

    pairs = [
        kernels(points, face_radius, face_angle, face_axial, face_stagger, face_area, n, 4, scale, passes // 2)
        for n in range(4)
    ]

    near = load([pltpu.with_memory_space_constraint(x, pltpu.HBM) for x in far])
    pairs, near, from_mid, from_plane = lax.optimization_barrier((pairs, near, from_mid, from_plane))
    flow_state, face_weights, forcing = [pltpu.with_memory_space_constraint(x, pltpu.VMEM) for x in near]
    to_left, to_right, own, other, index, gaps = edges(
        flow_state, face_weights, forcing, lagged_planes, face_map, from_mid, from_plane, phase_lag
    )
    from_left = lax.ppermute(to_right, "cell", rightward)
    from_right = lax.ppermute(to_left, "cell", leftward)
    state, to_left, to_right, surface, own, other, strip, rim = first_steps(
        flow_state, face_weights, forcing, gaps, from_mid, from_plane, from_left, from_right, own, other, index
    )
    surfaces = [surface]
    for level in range(2, STEPS, 2):
        from_left = lax.ppermute(to_right, "cell", rightward)
        from_right = lax.ppermute(to_left, "cell", leftward)
        got = next_steps(
            level, state, face_weights, forcing, from_left, from_right, own, other, strip, rim, index
        )
        if level < STEPS - 2:
            state, to_left, to_right, surface, own, other = got
        else:
            state, surface = got
        surfaces.append(surface)

    pieces = sound(
        [p[0] for p in pairs], [p[1] for p in pairs], surface_record, surfaces, observer_group[None, :]
    )
    part = jnp.sum(exchanged(pieces, ("x", "y_hi", "cell")), axis=0)
    part = jnp.sum(sent_to_all(part, "z"), axis=0)
    acoustic, array_signal = placed(sent_to_all(part, ("x", "y_hi")))
    return state, acoustic, array_signal


def solution(mesh):
    sizes = tuple(SPLIT.values())
    fine = Mesh(mesh.devices.reshape(*sizes, mesh.shape["cell"]), (*PASS, "cell"))
    return jax.shard_map(
        on_device,
        mesh=fine,
        in_specs=(
            P(PASS, "cell"),
            P(None, PASS, "cell"),
            P(PASS, "cell"),
            P(PASS, None, "cell"),
            P(),
            P(PASS, "cell"),
            P(PASS, None, "cell"),
            P(None, "cell"),
            P(None, "cell"),
            P(None, "cell"),
            P(None, "cell"),
            P(None, "cell"),
            P(),
            P(),
        ),
        out_specs=(P(PASS, "cell"), P("cell", None), P()),
        check_vma=False,
    )
```

```python
import functools
import math

import jax
import jax.numpy as jnp
from jax import lax
from jax.experimental import pallas as pl
from jax.experimental.pallas import tpu as pltpu
from jax.sharding import Mesh
from jax.sharding import PartitionSpec as P

STEPS = 8
GROUPS = 16
sound_speed = 2.0

W = 1024
E = 128
WX = W + E
TOP = 16 + 256
ROWS = TOP + 16
PACKED = 24
SPLIT = {"x": 4, "z": 8, "y_hi": 2, "y_lo": 2, "core": 2}
PASS = ("x", "z", "y_hi")
CELL = ("y_lo", "core")
VMEM_LIMIT = 8 * 1024 * 1024
F32 = jnp.float32
EDGE = jax.ShapeDtypeStruct((PACKED, E), F32)
HISTORY = jax.ShapeDtypeStruct((16, 8, 128), F32)
INDEX = jax.ShapeDtypeStruct((32, 128), jnp.int32)
GAPS = jax.ShapeDtypeStruct((16, W), F32)


def params(**kw):
    return pltpu.CompilerParams(vmem_limit_bytes=VMEM_LIMIT, **kw)


def vmem():
    return pl.BlockSpec(memory_space=pltpu.VMEM)


def place():
    index = lax.axis_index("x") * (SPLIT["z"] * SPLIT["y_hi"]) + lax.axis_index("z") * SPLIT["y_hi"]
    index = index + lax.axis_index("y_hi")
    return index // 2, index % 2


def strips_body(field, weights, forcing, lagged, maps, to_mid, to_plane, row, sems):
    _, half = place()
    mid = pl.multiple_of(jnp.where(half == 0, 248, 0), 8)
    plane = pl.multiple_of(jnp.where(half == 0, 0, 248), 8)
    copies = []
    for out, start in ((to_mid, mid), (to_plane, plane)):
        rows = pl.ds(start, 8)
        copies.append((field.at[rows], out.at[pl.ds(0, 8)]))
        for i in range(4):
            copies.append((weights.at[i, rows], out.at[pl.ds(8 + 8 * i, 8)]))
        copies.append((forcing.at[rows], out.at[pl.ds(40, 8)]))
    copies.append((lagged.at[0], to_plane.at[pl.ds(48, 8)]))
    copies.append((maps, row))
    started = []
    for n, (source, target) in enumerate(copies):
        copy = pltpu.make_async_copy(source, target, sems.at[n])
        copy.start()
        started.append(copy)
    for copy in started:
        copy.wait()
    sub = lax.broadcasted_iota(jnp.int32, (8, W), 0)
    to_plane[40:48, :] = jnp.where(sub == jnp.where(half == 0, 7, 0), row[...].astype(F32), to_plane[40:48, :])


def strips(field, weights, forcing, lagged, maps):
    anywhere = pl.BlockSpec(memory_space=pltpu.HBM)
    return pl.pallas_call(
        strips_body,
        out_shape=(jax.ShapeDtypeStruct((48, W), F32), jax.ShapeDtypeStruct((56, W), F32)),
        in_specs=[anywhere] * 5,
        out_specs=(vmem(), vmem()),
        scratch_shapes=[pltpu.VMEM((1, W), jnp.int32), pltpu.SemaphoreType.DMA((14,))],
        compiler_params=params(),
        name="strips",
    )(field, weights, forcing, lagged, maps)


def load_body(*refs):
    count = (len(refs) - 1) // 2
    copies = [pltpu.make_async_copy(refs[n], refs[count + n], refs[-1].at[n]) for n in range(count)]
    for copy in copies:
        copy.start()
    for copy in copies:
        copy.wait()


def load(arrays):
    count = len(arrays)
    return pl.pallas_call(
        load_body,
        out_shape=tuple(jax.ShapeDtypeStruct(a.shape, a.dtype) for a in arrays),
        in_specs=[pl.BlockSpec(memory_space=pltpu.HBM)] * count,
        out_specs=(vmem(),) * count,
        scratch_shapes=[pltpu.SemaphoreType.DMA((count,))],
        compiler_params=params(),
        cost_estimate=pl.CostEstimate(flops=0, bytes_accessed=12 << 20, transcendentals=0),
        name="load",
    )(*arrays)


def square(row):
    tiles = [row[:, 128 * s : 128 * (s + 1)] for s in range(8)]
    return jnp.concatenate(tiles, axis=0).astype(jnp.int32) & (W - 1)


def picked(history, level, lag, index):
    back = level - lag
    row = jnp.where(back >= 0, 8 + back, -back - 1)
    tiles = history[0]
    for n in range(1, 9 + level):
        tiles = jnp.where(row == n, history[n], tiles)
    high, low = index >> 7, index & 127
    out = jnp.zeros((8, 128), F32)
    for b in range(8):
        source = jnp.broadcast_to(tiles[b : b + 1, :], (8, 128))
        value = jnp.take_along_axis(source, low, axis=1, mode="promise_in_bounds")
        out = jnp.where(high == b, value, out)
    return out


def keep_lagged(history, lagged):
    for j in range(8):
        for b in range(8):
            history[j, b : b + 1, :] = lagged[j : j + 1, 128 * b : 128 * (b + 1)]


def fill_gaps(array, own, other, index, half, level):
    low = half == 0
    lanes = [slice(128 * b, 128 * (b + 1)) for b in range(8)]
    ends = [[array[r : r + 1, k] for k in lanes] for r in (7, 16, TOP - 1, TOP + 8)]
    for b in range(8):
        own[8 + level, b : b + 1, :] = jnp.where(low, ends[1][b], ends[2][b])
        other[8 + level, b : b + 1, :] = jnp.where(low, ends[0][b], ends[3][b])
    mine = picked(other, level, index[16:24, :], index[0:8, :])
    theirs = picked(own, level, index[24:32, :], index[8:16, :])
    for b, k in enumerate(lanes):
        array[15:16, k] = jnp.where(low, mine[b : b + 1], ends[0][b])
        array[8:9, k] = jnp.where(low, theirs[b : b + 1], ends[1][b])
        array[TOP : TOP + 1, k] = jnp.where(low, ends[3][b], mine[b : b + 1])
        array[TOP + 7 : TOP + 8, k] = jnp.where(low, ends[2][b], theirs[b : b + 1])


def lag_square(phase_lag, row, column):
    count, sides = phase_lag.shape
    at = lax.broadcasted_iota(jnp.int32, (count, sides), 0) == row
    at = at & (lax.broadcasted_iota(jnp.int32, (count, sides), 1) == column)
    lag = jnp.sum(jnp.where(at, phase_lag[...].astype(F32), 0.0), axis=0, keepdims=True)
    lag = jnp.sum(lag, axis=1, keepdims=True)
    return jnp.broadcast_to(lag, (8, 128)).astype(jnp.int32)


def set_index(index, maps, other_maps, phase_lag, passage, half):
    count = phase_lag.shape[0]
    index[0:8, :] = square(maps)
    index[8:16, :] = square(other_maps)
    index[16:24, :] = lag_square(phase_lag, passage, half)
    index[24:32, :] = lag_square(phase_lag, lax.rem(passage + 2 * half - 1 + count, count), 1 - half)


def relaxed(current, before, after, weights, forcing, width):
    sub = lax.broadcasted_iota(jnp.int32, (8, width), 0)
    inner = current[:, :width]
    below = jnp.where(sub == 0, pltpu.roll(before[:, :width], 1, 0), pltpu.roll(inner, 1, 0))
    above = jnp.where(sub == 7, pltpu.roll(after[:, :width], 7, 0), pltpu.roll(inner, 7, 0))
    left = pltpu.roll(current, 1, 1)[:, :width]
    right = pltpu.roll(current, WX - 1, 1)[:, :width]
    low = weights[0] * (below - inner) + weights[1] * (above - inner)
    side = weights[2] * (left - inner) + weights[3] * (right - inner)
    return (inner + forcing) + (low + side)


def step(source, target, weights, forcing, strip, rim, width, strips_too):
    def joined(own, edge):
        return own if width == W else jnp.concatenate([own, edge], axis=1)

    def one(start, row):
        own = pl.ds(row, 8)
        at = pl.ds(start, 8)
        w = [joined(weights[i, own, :], rim[i, at, :]) for i in range(4)]
        f = joined(forcing[own, :], rim[4, at, :])
        new = relaxed(
            source[at, :], source[pl.ds(start - 8, 8), :], source[pl.ds(start + 8, 8), :], w, f, width
        )
        return new

    def tile(t, carry):
        row = pl.multiple_of(8 * t, 8)
        start = pl.multiple_of(16 + 8 * t, 8)
        new = one(start, row)
        if target.shape[0] == ROWS:
            target[pl.ds(start, 8), :width] = new
        else:
            target[pl.ds(row, 8), :width] = new
        return carry

    lax.fori_loop(0, 32, tile, 0, unroll=True)
    if strips_too:
        for start, first, before, after in ((0, 0, 0, 8), (ROWS - 8, 8, ROWS - 16, ROWS - 8)):
            at = slice(start, start + 8)
            w = [joined(strip[i, first : first + 8, :], rim[i, at, :]) for i in range(4)]
            f = joined(strip[4, first : first + 8, :], rim[4, at, :])
            target[at, :width] = relaxed(
                source[at, :], source[before : before + 8, :], source[after : after + 8, :], w, f, width
            )


def strip_tiles(from_mid, from_plane, half, row, lanes):
    mid = from_mid[row : row + 8, lanes]
    plane = from_plane[row : row + 8, lanes]
    return jnp.where(half == 0, plane, mid), jnp.where(half == 0, mid, plane)


def packed_edge(block, sign):
    lane = lax.broadcasted_iota(jnp.int32, (PACKED, E), 1)
    spot = lane >> 3 if sign == 1 else 15 - (lane >> 3)
    out = jnp.zeros((PACKED, E), F32)
    for g in range(ROWS // PACKED):
        rows = block[PACKED * g : PACKED * (g + 1)]
        out = jnp.where(spot == g, pltpu.roll(rows, (sign * 8 * g) % E, 1) if g else rows, out)
    cell = lax.axis_index("y_lo") * SPLIT["core"] + lax.axis_index("core")
    end = 0 if sign == 1 else SPLIT["y_lo"] * SPLIT["core"] - 1
    return jnp.where(cell == end, 0.0, out)


def unpacked_edge(packed, sign):
    rows = [pltpu.roll(packed, (-sign * 8 * g) % E, 1) if g else packed for g in range(ROWS // PACKED)]
    return jnp.concatenate(rows, axis=0)


def edges_body(
    first, last, u_l, u_r, w_l, w_r, f_l, f_r, lagged, maps, from_mid, from_plane, phase_lag, to_left, to_right,
    own, other, index, gaps, array, wide,
):
    passage, half = place()
    full = slice(0, W)
    bottom, top = strip_tiles(from_mid, from_plane, half, 0, full)
    array[0:8, :] = bottom
    array[ROWS - 8 : ROWS, :] = top
    array[16:24, :] = first[...]
    array[TOP - 8 : TOP, :] = last[...]
    array[8:16, :] = jnp.zeros((8, W), F32)
    array[TOP : TOP + 8, :] = jnp.zeros((8, W), F32)
    keep_lagged(own, lagged.at[0])
    keep_lagged(other, from_plane.at[48:56])
    own[8:16] = jnp.zeros((8, 8, 128), F32)
    other[8:16] = jnp.zeros((8, 8, 128), F32)
    other_maps = jnp.where(half == 0, from_plane[40:41, :], from_plane[47:48, :])
    set_index(index, maps[...], other_maps, phase_lag, passage, half)
    fill_gaps(array, own, other, index, half, 0)
    gaps[0:8, :] = array[8:16, :]
    gaps[8:16, :] = array[TOP : TOP + 8, :]

    for out, block, u, w, f, sign in ((to_left, 0, u_l, w_l, f_l, 1), (to_right, 7, u_r, w_r, f_r, -1)):
        lanes = slice(128 * block, 128 * (block + 1))

        def packed(value, extra):
            lane = lax.broadcasted_iota(jnp.int32, value.shape, 1)
            for i, e in enumerate(extra):
                spot = 2 + i if sign == 1 else 125 - i
                value = jnp.where(lane == spot, pltpu.roll(e, (sign * (2 + i)) % 128, 1), value)
            return value

        wide[16:TOP, :] = packed(u[...], [w[0], w[1], w[2], w[3], f[...]])
        pairs = [strip_tiles(from_mid, from_plane, half, 8 * i, lanes) for i in range(6)]
        wide[0:8, :] = packed(pairs[0][0], [p[0] for p in pairs[1:]])
        wide[ROWS - 8 : ROWS, :] = packed(pairs[0][1], [p[1] for p in pairs[1:]])
        wide[8:16, :] = array[8:16, lanes]
        wide[TOP : TOP + 8, :] = array[TOP : TOP + 8, lanes]
        out[...] = packed_edge(wide[...], sign)


def edges(field, weights, forcing, lagged, maps, from_mid, from_plane, phase_lag):
    def spec(shape, *at):
        return pl.BlockSpec(shape, lambda i: at)

    whole = [spec((1, 8, W), 0, 0, 0), spec((1, W), 0, 0), spec((48, W), 0, 0), spec((56, W), 0, 0), spec((32, 2), 0, 0)]
    return pl.pallas_call(
        edges_body,
        grid=(1,),
        out_shape=(EDGE, EDGE, HISTORY, HISTORY, INDEX, GAPS),
        in_specs=[
            spec((8, W), 0, 0),
            spec((8, W), 31, 0),
            spec((256, E), 0, 0),
            spec((256, E), 0, 7),
            spec((4, 256, E), 0, 0, 0),
            spec((4, 256, E), 0, 0, 7),
            spec((256, E), 0, 0),
            spec((256, E), 0, 7),
            *whole,
        ],
        out_specs=(
            spec((PACKED, E), 0, 0), spec((PACKED, E), 0, 0), spec((16, 8, 128), 0, 0, 0), spec((16, 8, 128), 0, 0, 0),
            spec((32, 128), 0, 0), spec((16, W), 0, 0),
        ),
        scratch_shapes=[pltpu.VMEM((ROWS, W), F32), pltpu.VMEM((ROWS, E), F32)],
        compiler_params=params(),
        name="edges",
    )(field, field, field, field, weights, weights, forcing, forcing, lagged, maps, from_mid, from_plane, phase_lag)


def set_rim(array, left, right):
    lane = lax.broadcasted_iota(jnp.int32, (ROWS, E), 1)
    array[:, W:] = jnp.where(lane < 64, right, left)


def finish(level, source, between, out, surface, weights, forcing, strip, rim, own, other, index, half, tail):
    step(source, between, weights, forcing, strip, rim, WX, True)
    surface[0:1, :] = between[16 + 128 : 17 + 128, :W]
    fill_gaps(between, own, other, index, half, level + 1)
    step(between, out, weights, forcing, strip, rim, W, not tail)
    row = 128 if tail else 16 + 128
    surface[1:2, :] = out[row : row + 1, :]
    surface[2:8, :] = jnp.zeros((6, W), F32)


def first_body(
    field, weights, forcing, gaps, from_mid, from_plane, from_left, from_right, own_in, other_in, index,
    out, to_left, to_right, surface, own, other, strip, rim, source, between,
):
    _, half = place()
    full = slice(0, W)
    bottom, top = strip_tiles(from_mid, from_plane, half, 0, full)
    source[0:8, :W] = bottom
    source[ROWS - 8 : ROWS, :W] = top
    source[16:TOP, :W] = field[...]
    source[8:16, :W] = gaps[0:8, :]
    source[TOP : TOP + 8, :W] = gaps[8:16, :]
    left_edge, right_edge = unpacked_edge(from_left[...], -1), unpacked_edge(from_right[...], 1)
    set_rim(source, left_edge, right_edge)
    lane = lax.broadcasted_iota(jnp.int32, (ROWS, E), 1)
    for i in range(5):
        bottom, top = strip_tiles(from_mid, from_plane, half, 8 + 8 * i, full)
        strip[i, 0:8, :] = bottom
        strip[i, 8:16, :] = top
        right = pltpu.roll(right_edge, 128 - (2 + i), 1)
        left = pltpu.roll(left_edge, 2 + i, 1)
        rim[i, :, :] = jnp.where(lane == 0, right, jnp.where(lane == 127, left, 0.0))
    own[...] = own_in[...]
    other[...] = other_in[...]
    out[8:16, :] = jnp.zeros((8, W), F32)
    out[TOP : TOP + 8, :] = jnp.zeros((8, W), F32)
    between[8:16, :] = jnp.zeros((8, WX), F32)
    between[TOP : TOP + 8, :] = jnp.zeros((8, WX), F32)
    finish(0, source, between, out, surface, weights, forcing, strip, rim, own, other, index, half, False)
    fill_gaps(out, own, other, index, half, 2)
    to_left[...] = packed_edge(out[:, :E], 1)
    to_right[...] = packed_edge(out[:, W - E :], -1)


def next_body(
    level, tail, state, weights, forcing, from_left, from_right, own_in, other_in, strip, rim, index, *rest
):
    if tail:
        out, surface, own, other, source, between = rest
    else:
        out, to_left, to_right, surface, own, other, source, between = rest
    _, half = place()
    own[...] = own_in[...]
    other[...] = other_in[...]
    source[:, :W] = state[...]
    set_rim(source, unpacked_edge(from_left[...], -1), unpacked_edge(from_right[...], 1))
    between[8:16, :] = jnp.zeros((8, WX), F32)
    between[TOP : TOP + 8, :] = jnp.zeros((8, WX), F32)
    finish(level, source, between, out, surface, weights, forcing, strip, rim, own, other, index, half, tail)
    if not tail:
        out[8:16, :] = jnp.zeros((8, W), F32)
        out[TOP : TOP + 8, :] = jnp.zeros((8, W), F32)
        fill_gaps(out, own, other, index, half, level + 2)
        to_left[...] = packed_edge(out[:, :E], 1)
        to_right[...] = packed_edge(out[:, W - E :], -1)


STATE = jax.ShapeDtypeStruct((ROWS, W), F32)
BUFFERS = [pltpu.VMEM((ROWS, WX), F32), pltpu.VMEM((ROWS, WX), F32)]
COST = pl.CostEstimate(flops=2 * 16 * 330 * 1024, bytes_accessed=8 << 20, transcendentals=0)


def first_steps(field, weights, forcing, gaps, from_mid, from_plane, from_left, from_right, own, other, index):
    outs = (
        STATE, EDGE, EDGE, jax.ShapeDtypeStruct((8, W), F32), HISTORY, HISTORY,
        jax.ShapeDtypeStruct((5, 16, W), F32), jax.ShapeDtypeStruct((5, ROWS, E), F32),
    )
    return pl.pallas_call(
        first_body,
        out_shape=outs,
        in_specs=[vmem()] * 11,
        out_specs=tuple(vmem() for _ in outs),
        scratch_shapes=BUFFERS,
        compiler_params=params(),
        cost_estimate=COST,
        name="steps_first",
    )(field, weights, forcing, gaps, from_mid, from_plane, from_left, from_right, own, other, index)


def next_steps(level, state, weights, forcing, from_left, from_right, own, other, strip, rim, index):
    tail = level == STEPS - 2
    surface = jax.ShapeDtypeStruct((8, W), F32)
    if tail:
        outs = (jax.ShapeDtypeStruct((256, W), F32), surface)
        scratch = [pltpu.VMEM((16, 8, 128), F32), pltpu.VMEM((16, 8, 128), F32), *BUFFERS]
    else:
        outs = (STATE, EDGE, EDGE, surface, HISTORY, HISTORY)
        scratch = BUFFERS
    return pl.pallas_call(
        functools.partial(next_body, level, tail),
        out_shape=outs,
        in_specs=[vmem()] * 10,
        out_specs=tuple(vmem() for _ in outs),
        scratch_shapes=scratch,
        compiler_params=params(),
        cost_estimate=COST,
        name=f"steps_{level}",
    )(state, weights, forcing, from_left, from_right, own, other, strip, rim, index)


def kernels_body(points, radius, angle, axial, stagger, area, press, change, *, scale, passages):
    passage, half = place()

    def mine(ref):
        return jnp.where(half == 0, ref[0:1, :], ref[1:2, :])

    phase = passage.astype(F32) * (2.0 * math.pi / passages) + mine(angle)
    cos_phase, sin_phase = jnp.cos(phase), jnp.sin(phase)
    cos_stagger = jnp.cos(mine(stagger))
    weight = mine(area) * (scale / (4.0 * math.pi))
    normal_x = -weight * cos_stagger * sin_phase
    normal_y = weight * cos_stagger * cos_phase
    normal_z = weight * jnp.sin(mine(stagger))
    face_x = mine(radius) * cos_phase
    face_y = mine(radius) * sin_phase
    face_z = mine(axial)

    def tile(t, carry):
        rows = pl.ds(pl.multiple_of(16 * t, 16), 16)
        at = points[rows, :]
        delta_x = at[:, 0:1] - face_x
        delta_y = at[:, 1:2] - face_y
        delta_z = at[:, 2:3] - face_z
        inverse = lax.rsqrt(delta_x * delta_x + delta_y * delta_y + delta_z * delta_z)
        along = normal_x * delta_x + normal_y * delta_y + normal_z * delta_z
        both = along * inverse * inverse
        press[rows, :] = (both * inverse).astype(jnp.bfloat16)
        change[rows, :] = (both * (1.0 / sound_speed)).astype(jnp.bfloat16)
        return carry

    lax.fori_loop(0, press.shape[0] // 16, tile, 0, unroll=True)


def kernels(points, radius, angle, axial, stagger, area, part, count, scale, passages):
    size = points.shape[0] // count
    faces = pl.BlockSpec((2, W), lambda i: (0, 0))
    shape = jax.ShapeDtypeStruct((size, W), jnp.bfloat16)
    return pl.pallas_call(
        functools.partial(kernels_body, scale=scale, passages=passages),
        grid=(1,),
        out_shape=(shape, shape),
        in_specs=[pl.BlockSpec((size, 3), lambda i: (part, 0))] + [faces] * 5,
        out_specs=(pl.BlockSpec((size, W), lambda i: (0, 0)),) * 2,
        compiler_params=params(),
        cost_estimate=pl.CostEstimate(flops=20 * size * W, bytes_accessed=4 * size * W, transcendentals=size * W),
        name=f"kernels_{part}",
    )(points, radius, angle, axial, stagger, area)


def sound_body(*refs):
    presses, changes, (record, s0, s1, s2, s3, group, keep, give, total) = refs[:4], refs[4:8], refs[8:]
    late = jnp.concatenate([s[0:2, :] for s in (s0, s1, s2, s3)], axis=0).astype(jnp.bfloat16)
    surface = jnp.concatenate([record[0].astype(F32), late.astype(F32)], axis=0)
    times = surface.shape[0]
    row = lax.broadcasted_iota(jnp.int32, surface.shape, 0)
    after, before = pltpu.roll(surface, times - 1, 0), pltpu.roll(surface, 1, 0)
    first = row == 0
    last = row == times - 1
    rate = jnp.where(last, surface, after) - jnp.where(first, surface, before)
    rate = jnp.where(first | last, rate, rate * 0.5).astype(jnp.bfloat16)
    surface = surface.astype(jnp.bfloat16)
    turned = (((1,), (1,)), ((), ()))
    size = presses[0].shape[0]
    for n in range(4):
        got = lax.dot_general(presses[n][...], surface, turned, preferred_element_type=F32)
        got = got + lax.dot_general(changes[n][...], rate, turned, preferred_element_type=F32)
        total[size * n : size * (n + 1), :] = got
    label = lax.broadcasted_iota(jnp.int32, (GROUPS, group.shape[1]), 0)
    member = (group[...] == label).astype(F32)
    counts = jnp.sum(member, axis=1, keepdims=True)
    means = jnp.dot(member, total[...], precision=lax.Precision.HIGHEST, preferred_element_type=F32)
    means = means / jnp.maximum(counts, 1.0)
    core = lax.axis_index("core")
    for out, to in ((keep, core), (give, 1 - core)):
        for s in range(8):
            for c in range(2):
                start = pl.multiple_of(512 * c + 32 * s + 256 * to, 32)
                out[2 * s + c, 0:16] = total[pl.ds(start, 32), :].reshape(16, 2, 128)
                out[2 * s + c, 16] = means[2 * s : 2 * s + 2, :]


def sound(presses, changes, record, surfaces, group):
    return pl.pallas_call(
        sound_body,
        out_shape=(jax.ShapeDtypeStruct((16, 17, 2, 128), F32),) * 2,
        in_specs=[vmem()] * 14,
        out_specs=(vmem(), vmem()),
        scratch_shapes=[pltpu.VMEM((1024, 128), F32)],
        compiler_params=params(),
        name="sound",
    )(*presses, *changes, record, *surfaces, group)


def placed_body(parts, acoustic, array_signal):
    for s in range(8):
        acoustic[32 * s : 32 * (s + 1), :] = parts[s, 0:16].reshape(32, 128)
        array_signal[2 * s : 2 * s + 2, :] = parts[s, 16]


def placed(parts):
    return pl.pallas_call(
        placed_body,
        out_shape=(jax.ShapeDtypeStruct((256, 128), F32), jax.ShapeDtypeStruct((GROUPS, 128), F32)),
        in_specs=[vmem()],
        out_specs=(vmem(), vmem()),
        compiler_params=params(),
        name="placed",
    )(parts)


def store_body(state, after, out, sem):
    copy = pltpu.make_async_copy(state, out, sem)
    copy.start()
    copy.wait()


def store(state, after):
    return pl.pallas_call(
        store_body,
        out_shape=jax.ShapeDtypeStruct(state.shape, F32),
        in_specs=[vmem(), pl.BlockSpec(memory_space=pl.ANY)],
        out_specs=pl.BlockSpec(memory_space=pltpu.HBM),
        scratch_shapes=[pltpu.SemaphoreType.DMA],
        compiler_params=params(),
        cost_estimate=pl.CostEstimate(flops=0, bytes_accessed=2 << 20, transcendentals=0),
        name="store",
    )(pltpu.with_memory_space_constraint(state, pltpu.VMEM), after)


def merged_body(keep, got, after, out):
    out[...] = keep[...] + got[...]


def merged(keep, got, after):
    return pl.pallas_call(
        merged_body,
        out_shape=jax.ShapeDtypeStruct(keep.shape, F32),
        in_specs=[vmem(), vmem(), pl.BlockSpec(memory_space=pl.ANY)],
        out_specs=vmem(),
        compiler_params=params(),
        name="merged",
    )(keep, got, after)


def exchanged(pieces, axes):
    return lax.all_to_all(pieces, axes, 0, 0, tiled=True)


def sent_to_all(block, axes):
    count = lax.axis_size(axes)
    return exchanged(jnp.broadcast_to(block, (count, *block.shape)), axes)


def on_device(
    flow_state,
    face_weights,
    forcing,
    lagged_planes,
    phase_lag,
    face_map,
    surface_record,
    face_radius,
    face_angle,
    face_axial,
    face_stagger,
    face_area,
    listeners,
    observer_group,
):
    passes = lax.axis_size(PASS)
    cells = lax.axis_size(CELL)
    scale = 64.0 / math.sqrt(W * cells * passes)
    across = [(i, i ^ 1) for i in range(passes)]
    over = [(i, ((i + 1) ^ 1) - 1 if 0 < i < passes - 1 else passes - 1 - i) for i in range(passes)]
    rightward = [(i, (i + 1) % cells) for i in range(cells)]
    leftward = [(j, i) for i, j in rightward]

    far = (flow_state, face_weights, forcing, lagged_planes, face_map)
    to_mid, to_plane = strips(*[pltpu.with_memory_space_constraint(x, pltpu.HBM) for x in far])
    listeners, to_mid, to_plane, far = lax.optimization_barrier((listeners, to_mid, to_plane, far[:3]))
    points = listeners.T
    from_mid = lax.ppermute(to_mid, PASS, across)
    from_plane = lax.ppermute(to_plane, PASS, over)

    pairs = [
        kernels(points, face_radius, face_angle, face_axial, face_stagger, face_area, n, 4, scale, passes // 2)
        for n in range(4)
    ]

    near = load([pltpu.with_memory_space_constraint(x, pltpu.HBM) for x in far])
    pairs, near, from_mid, from_plane = lax.optimization_barrier((pairs, near, from_mid, from_plane))
    flow_state, face_weights, forcing = [pltpu.with_memory_space_constraint(x, pltpu.VMEM) for x in near]
    to_left, to_right, own, other, index, gaps = edges(
        flow_state, face_weights, forcing, lagged_planes, face_map, from_mid, from_plane, phase_lag
    )
    from_left = lax.ppermute(to_right, CELL, rightward)
    from_right = lax.ppermute(to_left, CELL, leftward)
    state, to_left, to_right, surface, own, other, strip, rim = first_steps(
        flow_state, face_weights, forcing, gaps, from_mid, from_plane, from_left, from_right, own, other, index
    )
    surfaces = [surface]
    for level in range(2, STEPS, 2):
        from_left = lax.ppermute(to_right, CELL, rightward)
        from_right = lax.ppermute(to_left, CELL, leftward)
        got = next_steps(
            level, state, face_weights, forcing, from_left, from_right, own, other, strip, rim, index
        )
        if level < STEPS - 2:
            state, to_left, to_right, surface, own, other = got
        else:
            state, surface = got
        surfaces.append(surface)

    keep, give = sound(
        [p[0] for p in pairs], [p[1] for p in pairs], surface_record, surfaces, observer_group[None, :]
    )
    state = store(state, keep)
    got = lax.ppermute(give, "core", [(0, 1), (1, 0)])
    pieces = merged(keep, got, pltpu.with_memory_space_constraint(state, pltpu.HBM))
    part = jnp.sum(exchanged(pieces, ("x", "y_hi", "y_lo")), axis=0)
    part = jnp.sum(sent_to_all(part, "z"), axis=0)
    acoustic, array_signal = placed(sent_to_all(part, ("x", "y_hi")))
    return state, acoustic, array_signal


def solution(mesh):
    fine = Mesh(mesh.devices.reshape(*SPLIT.values()), tuple(SPLIT))
    return jax.shard_map(
        on_device,
        mesh=fine,
        in_specs=(
            P(PASS, CELL),
            P(None, PASS, CELL),
            P(PASS, CELL),
            P(PASS, None, CELL),
            P(),
            P(PASS, CELL),
            P(PASS, None, CELL),
            P(None, CELL),
            P(None, CELL),
            P(None, CELL),
            P(None, CELL),
            P(None, CELL),
            P(),
            P(),
        ),
        out_specs=(P(PASS, CELL), P(CELL, None), P()),
        check_vma=False,
    )
```
